128 devices in a mesh: dp: 1, tp: 2 (over core), sp: 64 (over z, y, x).
Axes of the slice: x: 4, y: 4, z: 4, core: 2. Of those that a mesh axis runs over, the one named last changes fastest.
Arguments:
- hidden: bfloat16 [32, 6144], P('dp')
- norm_scale: bfloat16 [6144], replicated
- w_qkv: bfloat16 [6144, 8192], P(None, 'tp')
- w_out: bfloat16 [6144, 6144], P('tp')
- k_cache: bfloat16 [32, 4096, 8, 128], P('dp', 'sp', 'tp')
- v_cache: bfloat16 [32, 4096, 8, 128], P('dp', 'sp', 'tp')
- positions: int32 [32], P('dp')
Outputs:
- output 1: bfloat16 [32, 6144], P('dp')
- output 2: bfloat16 [32, 4096, 8, 128], P('dp', 'sp', 'tp')
- output 3: bfloat16 [32, 4096, 8, 128], P('dp', 'sp', 'tp')
All inputs are finite; a program needn't handle non-finite values.
Results may differ from the reference program's by a relative error of at most 0.00522225.
Values sent between devices are 32-bit elements.
A program may use at most 1 GiB of HBM per device.

```python
import math
import jax
import jax.numpy as jnp
from jax import lax

BATCH = 32
SEQ = 4096
D = 6144
HEADS = 48
KV_HEADS = 8
HEAD = 128


def rope_apply(head_vals, positions):
    half_dim = head_vals.shape[-1] // 2
    inv_freq = jnp.exp(jnp.arange(half_dim, dtype=jnp.float32) * (-2.0 * math.log(500000.0) / head_vals.shape[-1]))
    angles = positions.astype(jnp.float32)[:, None] * inv_freq[None, :]
    cos_part = jnp.cos(angles)[:, None, None, :]
    sin_part = jnp.sin(angles)[:, None, None, :]
    first_half = head_vals[..., :half_dim]
    second_half = head_vals[..., half_dim:]
    return jnp.concatenate([first_half * cos_part - second_half * sin_part, second_half * cos_part + first_half * sin_part], axis=-1)


def setup_inputs(seed: int = 0, part: int = 0) -> dict:
    part_keys = jax.random.split(jax.random.fold_in(jax.random.key(seed), part), 5)
    shared_keys = jax.random.split(jax.random.key(seed + 1), 4)
    qkv_width = (HEADS + 2 * KV_HEADS) * HEAD
    hidden = jax.random.normal(part_keys[0], (BATCH, D), jnp.float32)
    norm_scale = 1.0 + 0.5 * jax.random.normal(shared_keys[0], (D,), jnp.float32)
    col_boost = jnp.where(jax.random.randint(shared_keys[1], (qkv_width,), 0, 16) == 0, 10.0, 1.0)
    w_qkv = jax.random.normal(shared_keys[2], (D, qkv_width), jnp.float32) * col_boost * (D ** -0.5)
    w_out = jax.random.normal(shared_keys[3], (HEADS * HEAD, D), jnp.float32) * (2.0 * (HEADS * HEAD) ** -0.5)
    k_cache = 0.5 * jax.random.normal(part_keys[1], (BATCH, SEQ, KV_HEADS, HEAD), jnp.float32)
    coarse = jax.random.normal(part_keys[2], (BATCH, 8, 1, KV_HEADS, HEAD), jnp.float32)
    fine_part = jax.random.normal(part_keys[3], (BATCH, 8, SEQ // 8, KV_HEADS, HEAD), jnp.float32)
    v_cache = (coarse + 0.5 * fine_part).reshape(BATCH, SEQ, KV_HEADS, HEAD)
    positions = jax.random.randint(part_keys[4], (BATCH,), SEQ // 8, SEQ)
    positions = positions.at[0].set(SEQ - 1).at[1].set(SEQ // 8)
    return {
        'hidden': hidden.astype(jnp.bfloat16),
        'norm_scale': norm_scale.astype(jnp.bfloat16),
        'w_qkv': w_qkv.astype(jnp.bfloat16),
        'w_out': w_out.astype(jnp.bfloat16),
        'k_cache': k_cache.astype(jnp.bfloat16),
        'v_cache': v_cache.astype(jnp.bfloat16),
        'positions': positions.astype(jnp.int32),
    }


def reference(hidden, norm_scale, w_qkv, w_out, k_cache, v_cache, positions):
    q_per_kv = HEADS // KV_HEADS
    hidden_f32 = hidden.astype(jnp.float32)
    row_mean = jnp.mean(hidden_f32, axis=-1, keepdims=True)
    centered = hidden_f32 - row_mean
    row_var = jnp.mean(centered * centered, axis=-1, keepdims=True)
    normed = (centered * lax.rsqrt(row_var + 1e-5) * norm_scale.astype(jnp.float32)).astype(jnp.bfloat16)
    qkv_proj = jnp.clip(jnp.dot(normed, w_qkv, preferred_element_type=jnp.float32).astype(jnp.bfloat16), -8.0, 8.0)
    grouped = qkv_proj.reshape(BATCH, KV_HEADS, q_per_kv + 2, HEAD)
    rotated = rope_apply(grouped[:, :, : q_per_kv + 1].astype(jnp.float32), positions).astype(jnp.bfloat16)
    queries = rotated[:, :, :q_per_kv]
    new_row = (jnp.arange(SEQ)[None, :] == positions[:, None])[:, :, None, None]
    k_upd = jnp.where(new_row, rotated[:, :, q_per_kv][:, None], k_cache)
    v_upd = jnp.where(new_row, grouped[:, :, q_per_kv + 1][:, None], v_cache)

    def one_sequence(seq_args):
        q_seq, k_seq, v_seq, p_seq = seq_args
        scores = jnp.einsum('gqd,sgd->gqs', q_seq.astype(jnp.float32), k_seq.astype(jnp.float32)) * (HEAD ** -0.5)
        valid_mask = jnp.arange(SEQ) <= p_seq
        scores = jnp.where(valid_mask[None, None, :], scores, -jnp.inf)
        weights_bf = jax.nn.softmax(scores, axis=-1).astype(jnp.bfloat16)
        return jnp.einsum('gqs,sgd->gqd', weights_bf.astype(jnp.float32), v_seq.astype(jnp.float32))

    attn_out = lax.map(one_sequence, (queries, k_upd, v_upd, positions))
    attn_flat = attn_out.reshape(BATCH, HEADS * HEAD).astype(jnp.bfloat16)
    h_out = (hidden_f32 + jnp.dot(attn_flat, w_out, preferred_element_type=jnp.float32)).astype(jnp.bfloat16)
    return (h_out, k_upd, v_upd)
```

```python
import functools
import math

import jax
import jax.numpy as jnp
from jax import lax
from jax.experimental import pallas as pl
from jax.experimental.pallas import tpu as pltpu
from jax.sharding import PartitionSpec as P

MESH = pl.DeviceIdType.MESH
VMEM = pltpu.VMEM
F32 = jnp.float32
BF16 = jnp.bfloat16
NEG = -3.0e38
PLANE = 16
K_CHUNKS = 6


def qkv_kernel(h_ref, scale_ref, cos_ref, sin_ref, w_ref, x_ref,
               w_buf, recv, xs, w_sem, send_sem, recv_sem):
    sp = lax.axis_index("sp")
    j = lax.rem(sp, PLANE)
    base = sp - j
    n_seq, d_model = h_ref.shape
    width = w_buf.shape[1]
    rows = d_model // K_CHUNKS
    cols = pl.ds(pl.multiple_of(j * width, width), width)

    def w_copy(c):
        return pltpu.make_async_copy(
            w_ref.at[pl.ds(c * rows, rows), cols], w_buf.at[pl.ds(c * rows, rows)], w_sem.at[c])

    for c in range(K_CHUNKS):
        w_copy(c).start()
    barrier = pltpu.get_barrier_semaphore()

    def greet(d, carry):
        pl.semaphore_signal(barrier, inc=1, device_id={"sp": base + lax.rem(j + d, PLANE)}, device_id_type=MESH)
        return carry

    lax.fori_loop(1, PLANE, greet, 0)

    hidden = h_ref[...].astype(F32)
    centered = hidden - jnp.mean(hidden, axis=-1, keepdims=True)
    var = jnp.mean(centered * centered, axis=-1, keepdims=True)
    u = (centered * lax.rsqrt(var + 1e-5) * scale_ref[...].astype(F32)).astype(BF16)
    acc = jnp.zeros((n_seq, width), F32)
    for c in range(K_CHUNKS):
        w_copy(c).wait()
        acc += jnp.dot(u[:, c * rows:(c + 1) * rows], w_buf[c * rows:(c + 1) * rows, :],
                       preferred_element_type=F32)
    y = jnp.clip(acc.astype(BF16), -8.0, 8.0).astype(F32)
    heads = []
    is_kv = lax.rem(j, 4) == 3
    for i in range(width // 128):
        part = y[:, i * 128:(i + 1) * 128]
        swapped = pltpu.roll(part, 64, 1)
        turned = (part * cos_ref[...] + swapped * sin_ref[...]).astype(BF16).astype(F32)
        heads.append(turned if i == 0 else jnp.where(is_kv, part, turned))
    recv[j] = jnp.concatenate(heads, axis=1)
    pl.semaphore_wait(barrier, PLANE - 1)

    def send(d):
        return pltpu.make_async_remote_copy(
            src_ref=recv.at[j], dst_ref=recv.at[j], send_sem=send_sem, recv_sem=recv_sem,
            device_id={"sp": base + lax.rem(j + d, PLANE)}, device_id_type=MESH)

    def start(d, carry):
        send(d).start()
        return carry

    lax.fori_loop(1, PLANE, start, 0)
    others = recv.at[pl.ds(0, PLANE - 1)]
    pltpu.make_async_copy(others, others, recv_sem).wait()
    for blk in range(PLANE):
        for i in range(width // 128):
            xs[pl.ds(blk * (width // 128) + i, n_seq, stride=32), :] = recv[blk, :, i * 128:(i + 1) * 128]
    x_ref[...] = xs[...].astype(BF16)
    pltpu.make_async_copy(others, others, send_sem).wait()


def attn_kernel(pos_ref, x_ref, k_ref, v_ref, o_ref, k_out, v_out, k_buf, v_buf, in_sem, out_sem):
    n_seq, n_rows, head_dim = k_ref.shape
    kv = 4
    seq_local = n_rows // kv
    base = lax.axis_index("sp") * seq_local
    steps, per = 8, n_seq // 8

    def load(c, which):
        src, dst = ((k_ref, k_buf), (v_ref, v_buf))[which]
        return pltpu.make_async_copy(src.at[pl.ds(c * per, per)], dst.at[pl.ds(c * per, per)], in_sem.at[which, c])

    def store(c, which):
        src, dst = ((k_buf, k_out), (v_buf, v_out))[which]
        return pltpu.make_async_copy(src.at[pl.ds(c * per, per)], dst.at[pl.ds(c * per, per)], out_sem.at[which, c])

    for c in range(steps):
        load(c, 0).start()
        load(c, 1).start()
    row = lax.broadcasted_iota(jnp.int32, (32, n_rows), 0)
    col = lax.broadcasted_iota(jnp.int32, (32, n_rows), 1)
    seq_of = jnp.where(col % kv == row // 8, col // kv + base, 1 << 30)
    row8 = lax.broadcasted_iota(jnp.int32, (32, head_dim), 0) % 8
    diag = lax.broadcasted_iota(jnp.int32, (32, head_dim), 1) == row8
    slab_row = lax.broadcasted_iota(jnp.int32, (n_rows, head_dim), 0)
    scale = head_dim ** -0.5

    def spread(col_vec):
        tiles = jnp.where(diag, col_vec, 0.0).reshape(4, 8, head_dim)
        return jnp.broadcast_to(jnp.sum(tiles, axis=1, keepdims=True), (4, 8, head_dim)).reshape(32, head_dim)

    for c in range(steps):
        load(c, 0).wait()
        load(c, 1).wait()
        for i in range(per):
            b = c * per + i
            p = pos_ref[b]
            xb = x_ref[pl.ds(b * 32, 32), :]

            @pl.when(jnp.logical_and(p >= base, p < base + seq_local))
            def _():
                xf = xb.astype(F32)
                for buf, r in ((k_buf, 6), (v_buf, 7)):
                    new = jnp.zeros((n_rows, head_dim), F32)
                    for g in range(kv):
                        new = jnp.where(slab_row % kv == g, xf[g * 8 + r:g * 8 + r + 1, :], new)
                    buf[b] = jnp.where(slab_row // kv + base == p, new, buf[b].astype(F32)).astype(BF16)

            s = lax.dot_general(xb, k_buf[b], (((1,), (1,)), ((), ())), preferred_element_type=F32) * scale
            s = jnp.where(seq_of <= p, s, NEG)
            m = jnp.max(s, axis=1, keepdims=True)
            e = jnp.exp(s - m)
            l = jnp.sum(e, axis=1, keepdims=True)
            o = jnp.dot(e.astype(BF16), v_buf[b], preferred_element_type=F32)
            o = jnp.where(row8 == 6, spread(m), jnp.where(row8 == 7, spread(l), o))
            o_ref[pl.ds(b * 4, 4)] = o.reshape(4, 8, head_dim)
        store(c, 0).start()
        store(c, 1).start()
    for c in range(steps):
        store(c, 0).wait()
        store(c, 1).wait()


def merge_kernel(n_sp, o_ref, h_ref, w_ref, out_ref, parts, w_buf, lhs, mine, shares, full, other,
                 w_sem, rs_send, rs_recv, x_send, x_recv, ag_send, ag_recv, tp_send, tp_recv):
    sp = lax.axis_index("sp")
    tp = lax.axis_index("tp")
    line, group = lax.div(sp, 4), lax.rem(sp, 4)
    depth = w_buf.shape[0]
    width = 768
    n_own = 8

    def w_copy(c):
        return pltpu.make_async_copy(
            w_ref.at[pl.ds(pl.multiple_of(group * depth, depth), depth), pl.ds(c * width, width)],
            w_buf.at[:, pl.ds(c * width, width)], w_sem.at[c])

    for c in range(n_own):
        w_copy(c).start()

    barrier = pltpu.get_barrier_semaphore()

    def greet(d, carry):
        pl.semaphore_signal(barrier, inc=1, device_id={"sp": lax.rem(sp + d, n_sp)}, device_id_type=MESH)
        return carry

    lax.fori_loop(1, n_sp, greet, 0)
    for d in range(4):
        pl.semaphore_signal(barrier, inc=1, device_id={"tp": 1 - tp, "sp": line * 4 + lax.rem(group + d, 4)},
                            device_id_type=MESH)
    pl.semaphore_wait(barrier, n_sp - 1 + 4)

    def rs(d):
        peer = lax.rem(sp + d, n_sp)
        return pltpu.make_async_remote_copy(
            src_ref=o_ref.at[lax.div(peer, 4), :, lax.rem(peer, 4)], dst_ref=parts.at[sp], send_sem=rs_send,
            recv_sem=rs_recv, device_id={"sp": peer}, device_id_type=MESH)

    def rs_start(d, carry):
        rs(d).start()
        return carry

    lax.fori_loop(1, n_sp, rs_start, 0)
    parts[sp] = o_ref[line, :, group]
    others = parts.at[pl.ds(0, n_sp - 1)]
    pltpu.make_async_copy(others, others, rs_recv).wait()

    lane = lax.broadcasted_iota(jnp.int32, (1, 128), 1)
    lhs[...] = jnp.zeros_like(lhs)
    for t in range(2):
        m = parts[:, t, 6, :]
        l = parts[:, t, 7, :]
        f = jnp.exp(m - jnp.max(m, axis=0, keepdims=True))
        den = jnp.sum(f * l, axis=0, keepdims=True)
        wt = (f / jnp.where(lane < 6, den, 1.0)).T
        acc = jnp.zeros((8, 128), F32)
        for s in range(n_sp):
            acc += wt[:8, s:s + 1] * parts[s, t]
        for hd in range(6):
            lhs[t:t + 1, hd * 128:(hd + 1) * 128] = acc[hd:hd + 1, :]

    me = group * 2 + tp
    left = lhs[...].astype(BF16)
    for c in range(n_own):
        w_copy(c).wait()
        res = jnp.dot(left, w_buf[:, c * width:(c + 1) * width], preferred_element_type=F32)
        for t in range(2):
            for cb in range(6):
                mine[c, t, cb:cb + 1, :] = res[t:t + 1, cb * 128:(cb + 1) * 128]

    def x_copy(d):
        owner = lax.rem(me + d, n_own)
        return pltpu.make_async_remote_copy(
            src_ref=mine.at[owner], dst_ref=shares.at[me], send_sem=x_send, recv_sem=x_recv,
            device_id={"tp": lax.rem(owner, 2), "sp": line * 4 + lax.div(owner, 2)}, device_id_type=MESH)

    for d in range(1, n_own):
        x_copy(d).start()
    shares[me] = mine[me]
    x_others = shares.at[pl.ds(0, n_own - 1)]
    pltpu.make_async_copy(x_others, x_others, x_recv).wait()
    slot = group * (n_sp // 4) + line
    total = shares[0]
    for s in range(1, n_own):
        total += shares[s]
    full[slot] = total

    def ag(d):
        return pltpu.make_async_remote_copy(
            src_ref=full.at[slot], dst_ref=full.at[slot], send_sem=ag_send, recv_sem=ag_recv,
            device_id={"sp": lax.rem(sp + d, n_sp)}, device_id_type=MESH)

    def ag_start(d, carry):
        ag(d).start()
        return carry

    lax.fori_loop(1, n_sp, ag_start, 0)
    f_others = full.at[pl.ds(0, n_sp - 1)]
    pltpu.make_async_copy(f_others, f_others, ag_recv).wait()
    swap = pltpu.make_async_remote_copy(
        src_ref=full, dst_ref=other, send_sem=tp_send, recv_sem=tp_recv, device_id={"tp": 1 - tp},
        device_id_type=MESH)
    swap.start()

    def finish(buf, core):
        for g in range(4):
            for cb in range(6):
                slab = jnp.concatenate(
                    [buf[pl.ds(g * 16 + q * 4, 4), :, cb, :].reshape(8, 128) for q in range(4)], axis=0)
                at = pl.ds(pl.multiple_of((g * 2 + core) * width + cb * 128, 128), 128)
                out_ref[:, at] = (h_ref[:, at].astype(F32) + slab).astype(BF16)

    finish(full, tp)
    swap.wait()
    finish(other, 1 - tp)
    pltpu.make_async_copy(others, others, rs_send).wait()
    pltpu.make_async_copy(x_others, x_others, x_send).wait()
    pltpu.make_async_copy(f_others, f_others, ag_send).wait()


def solution(mesh):
    cache_spec = P('dp', 'sp', 'tp', None)
    n_sp = mesh.shape["sp"]

    def local_step(hidden, norm_scale, w_qkv, w_out, k_cache, v_cache, positions):
        n_seq, seq_local, kv, head_dim = k_cache.shape
        d_model = hidden.shape[1]
        width = w_qkv.shape[1] // PLANE
        vmem = pl.BlockSpec(memory_space=VMEM)
        anyspace = pl.BlockSpec(memory_space=pl.ANY)
        half = head_dim // 2
        inv_freq = jnp.exp(jnp.arange(half, dtype=F32) * (-2.0 * math.log(500000.0) / head_dim))
        angles = positions.astype(F32)[:, None] * inv_freq[None, :]
        cos, sin = jnp.cos(angles), jnp.sin(angles)
        cos = jnp.concatenate([cos, cos], axis=1)
        sin = jnp.concatenate([-sin, sin], axis=1)

        x = pl.pallas_call(
            qkv_kernel,
            out_shape=jax.ShapeDtypeStruct((n_seq * 32, head_dim), BF16),
            in_specs=[vmem, vmem, vmem, vmem, anyspace],
            out_specs=vmem,
            scratch_shapes=[
                VMEM((d_model, width), BF16),
                VMEM((PLANE, n_seq, width), F32),
                VMEM((n_seq * 32, head_dim), F32),
                pltpu.SemaphoreType.DMA((K_CHUNKS,)),
                pltpu.SemaphoreType.DMA,
                pltpu.SemaphoreType.DMA,
            ],
            compiler_params=pltpu.CompilerParams(collective_id=0, has_side_effects=True),
            name="qkv",
        )(hidden, norm_scale.reshape(1, d_model), cos, sin, w_qkv)

        rows = seq_local * kv
        flat = (n_seq, rows, head_dim)
        o, k_new, v_new = pl.pallas_call(
            attn_kernel,
            out_shape=[
                jax.ShapeDtypeStruct((n_seq * kv, 8, head_dim), F32),
                jax.ShapeDtypeStruct(flat, BF16),
                jax.ShapeDtypeStruct(flat, BF16),
            ],
            in_specs=[pl.BlockSpec(memory_space=pltpu.SMEM), vmem, anyspace, anyspace],
            out_specs=[vmem, anyspace, anyspace],
            scratch_shapes=[
                VMEM(flat, BF16),
                VMEM(flat, BF16),
                pltpu.SemaphoreType.DMA((2, 8)),
                pltpu.SemaphoreType.DMA((2, 8)),
            ],
            name="attn",
        )(positions, x, k_cache.reshape(flat), v_cache.reshape(flat))

        depth = w_out.shape[0] // kv
        h_out = pl.pallas_call(
            functools.partial(merge_kernel, n_sp),
            out_shape=jax.ShapeDtypeStruct((n_seq, d_model), BF16),
            in_specs=[vmem, vmem, anyspace],
            out_specs=vmem,
            scratch_shapes=[
                VMEM((n_sp, 2, 8, head_dim), F32),
                VMEM((depth, d_model), BF16),
                VMEM((8, depth), F32),
                VMEM((8, 2, 8, head_dim), F32),
                VMEM((8, 2, 8, head_dim), F32),
                VMEM((n_sp, 2, 8, head_dim), F32),
                VMEM((n_sp, 2, 8, head_dim), F32),
                pltpu.SemaphoreType.DMA((8,)),
            ] + [pltpu.SemaphoreType.DMA] * 8,
            compiler_params=pltpu.CompilerParams(collective_id=1, has_side_effects=True),
            name="merge",
        )(o.reshape(n_seq // 2, 2, kv, 8, head_dim), hidden, w_out)
        return h_out, k_new.reshape(k_cache.shape), v_new.reshape(v_cache.shape)

    return jax.shard_map(
        local_step,
        mesh=mesh,
        in_specs=(P('dp', None), P(None), P(None, 'tp'), P('tp', None), cache_spec, cache_spec, P('dp')),
        out_specs=(P('dp', None), cache_spec, cache_spec),
        check_vma=False,
    )
```

```python
import functools
import math

import jax
import jax.numpy as jnp
import numpy as np
from jax import lax
from jax.experimental import pallas as pl
from jax.experimental.pallas import tpu as pltpu
from jax.sharding import PartitionSpec as P

MESH = pl.DeviceIdType.MESH
VMEM = pltpu.VMEM
F32 = jnp.float32
BF16 = jnp.bfloat16
NEG = -3.0e38
PLANE = 16
K_CHUNKS = 6
KV = 4
OWNERS = 8


def step_kernel(pos_hbm, h_hbm, scale_hbm, freq_hbm, wq_ref, wo_ref, k_ref, v_ref, out_ref, new_ref,
                pos_ref, h_ref, scale_ref, freq_ref, in_sem, wq_buf, wo_buf, k_buf, v_buf, recv, xs, xb, part, parts, lhs, mine, shares, full, other,
                wq_sem, wo_sem, kv_sem, q_send, q_recv, rs_send, rs_recv, x_send, x_recv,
                ag_send, ag_recv, tp_send, tp_recv):
    sp = lax.axis_index("sp")
    tp = lax.axis_index("tp")
    n_sp = 64
    line, group = lax.div(sp, KV), lax.rem(sp, KV)
    n_lines = n_sp // KV
    j = lax.rem(sp, PLANE)
    base = sp - j
    n_seq, d_model = h_ref.shape
    width = wq_buf.shape[1]
    heads_per = width // 128
    rows = d_model // K_CHUNKS
    n_rows = k_ref.shape[1]
    seq_local = n_rows // KV
    depth = wo_buf.shape[0]
    own = d_model // OWNERS
    n_cb = own // 128

    def wq_copy(c):
        return pltpu.make_async_copy(
            wq_ref.at[pl.ds(c * rows, rows), pl.ds(pl.multiple_of(j * width, width), width)],
            wq_buf.at[pl.ds(c * rows, rows)], wq_sem.at[c])

    def wo_copy(c):
        return pltpu.make_async_copy(
            wo_ref.at[pl.ds(pl.multiple_of(group * depth, depth), depth), pl.ds(c * own, own)],
            wo_buf.at[:, pl.ds(c * own, own)], wo_sem.at[c])

    k_copy = pltpu.make_async_copy(k_ref, k_buf, kv_sem.at[0])
    v_copy = pltpu.make_async_copy(v_ref, v_buf, kv_sem.at[1])
    small = [pltpu.make_async_copy(src, dst, in_sem.at[i]) for i, (src, dst) in enumerate(
        [(h_hbm, h_ref), (pos_hbm, pos_ref), (freq_hbm, freq_ref), (scale_hbm, scale_ref)])]
    for c in small:
        c.start()
    for c in range(K_CHUNKS):
        wq_copy(c).start()
    k_copy.start()
    v_copy.start()
    for c in range(OWNERS):
        wo_copy(c).start()

    barrier = pltpu.get_barrier_semaphore()

    def greet(d, carry):
        pl.semaphore_signal(barrier, inc=1, device_id={"sp": lax.rem(sp + d, n_sp)}, device_id_type=MESH)
        return carry

    with jax.named_scope("greet"):
        lax.fori_loop(1, n_sp, greet, 0)
        for d in range(KV):
            pl.semaphore_signal(barrier, inc=1, device_id={"tp": 1 - tp, "sp": line * KV + lax.rem(group + d, KV)},
                                device_id_type=MESH)

    with jax.named_scope("inwait"):
        for c in small:
            c.wait()
    with jax.named_scope("norm"):
        seq_row = lax.broadcasted_iota(jnp.int32, (n_seq, 128), 0)
        pos = jnp.zeros((n_seq, 128), jnp.int32)
        for b in range(n_seq):
            pos = jnp.where(seq_row == b, pos_ref[b], pos)
        angles = pos.astype(F32) * freq_ref[...]
        cos = jnp.cos(angles)
        sin = jnp.sin(angles)
        sin = jnp.where(lax.broadcasted_iota(jnp.int32, (n_seq, 128), 1) < 64, -sin, sin)
        hidden = h_ref[...].astype(F32)
        centered = hidden - jnp.mean(hidden, axis=-1, keepdims=True)
        var = jnp.mean(centered * centered, axis=-1, keepdims=True)
        u = (centered * lax.rsqrt(var + 1e-5) * scale_ref[...].astype(F32)[None, :]).astype(BF16)

    with jax.named_scope("qkv"):
        acc = jnp.zeros((n_seq, width), F32)
        for c in range(K_CHUNKS):
            wq_copy(c).wait()
            acc += jnp.dot(u[:, c * rows:(c + 1) * rows], wq_buf[c * rows:(c + 1) * rows, :],
                           preferred_element_type=F32)
        y = jnp.clip(acc.astype(BF16), -8.0, 8.0).astype(F32)
        heads = []
        is_kv = lax.rem(j, 4) == 3
        for i in range(heads_per):
            piece = y[:, i * 128:(i + 1) * 128]
            turned = (piece * cos + pltpu.roll(piece, 64, 1) * sin).astype(BF16).astype(F32)
            heads.append(turned if i == 0 else jnp.where(is_kv, piece, turned))
        recv[j] = jnp.concatenate(heads, axis=1)
    with jax.named_scope("barrier"):
        pl.semaphore_wait(barrier, n_sp - 1 + KV)

    def q_start(d, carry):
        pltpu.make_async_remote_copy(
            src_ref=recv.at[j], dst_ref=recv.at[j], send_sem=q_send, recv_sem=q_recv,
            device_id={"sp": base + lax.rem(j + d, PLANE)}, device_id_type=MESH).start()
        return carry

    with jax.named_scope("qsend"):
        lax.fori_loop(1, PLANE, q_start, 0)
    q_others = recv.at[pl.ds(0, PLANE - 1)]
    with jax.named_scope("qwait"):
        pltpu.make_async_copy(q_others, q_others, q_recv).wait()
    with jax.named_scope("spread"):
        for blk in range(PLANE):
            for i in range(heads_per):
                xs[pl.ds(blk * heads_per + i, n_seq, stride=32), :] = recv[blk, :, i * 128:(i + 1) * 128]
        xb[...] = xs[...].astype(BF16)
        new_ref[...] = xb[...]

    row8 = lax.broadcasted_iota(jnp.int32, (32, 128), 0) % 8
    diag = lax.broadcasted_iota(jnp.int32, (32, 128), 1) == row8

    def spread(col_vec, n):
        tiles = jnp.where(diag[:8 * n], col_vec, 0.0).reshape(n, 8, 128)
        return jnp.broadcast_to(jnp.sum(tiles, axis=1, keepdims=True), (n, 8, 128)).reshape(8 * n, 128)

    with jax.named_scope("kvwait"):
        k_copy.wait()
        v_copy.wait()
    row = lax.broadcasted_iota(jnp.int32, (32, n_rows), 0)
    col = lax.broadcasted_iota(jnp.int32, (32, n_rows), 1)
    seq_of = jnp.where(col % KV == row // 8, col // KV + sp * seq_local, 1 << 30)
    scale = 128 ** -0.5
    with jax.named_scope("attn"):
        for i in range(1, n_lines + 1):
            ln = lax.rem(line + i, n_lines)
            for t in range(2):
                b = ln * 2 + t
                q = xb[pl.ds(pl.multiple_of(b * 32, 32), 32), :]
                s = lax.dot_general(q, k_buf[b], (((1,), (1,)), ((), ())), preferred_element_type=F32) * scale
                s = jnp.where(seq_of < pos_ref[b], s, NEG)
                m = jnp.max(s, axis=1, keepdims=True)
                e = jnp.exp(s - m)
                l = jnp.sum(e, axis=1, keepdims=True)
                o = jnp.dot(e.astype(BF16), v_buf[b], preferred_element_type=F32)
                o = jnp.where(row8 == 6, spread(m, KV), jnp.where(row8 == 7, spread(l, KV), o))
                part[ln, :, t] = o.reshape(KV, 8, 128)
            for d in range(KV):
                if i == n_lines and d == 0:
                    continue
                to = lax.rem(group + d, KV)
                pltpu.make_async_remote_copy(
                    src_ref=part.at[ln, to], dst_ref=parts.at[sp], send_sem=rs_send, recv_sem=rs_recv,
                    device_id={"sp": ln * KV + to}, device_id_type=MESH).start()
        parts[sp] = part[line, group]

    with jax.named_scope("newrow"):
        fresh = []
        for t in range(2):
            tile = xs[pl.ds(pl.multiple_of((line * 2 + t) * 32 + group * 8, 8), 8), :]
            score = jnp.sum(tile * tile[6:7, :], axis=1, keepdims=True) * scale
            fresh.append((spread(score, 1)[:1], tile[7:8, :]))

    others = parts.at[pl.ds(0, n_sp - 1)]
    with jax.named_scope("rswait"):
        pltpu.make_async_copy(others, others, rs_recv).wait()
    with jax.named_scope("merge"):
        lane = lax.broadcasted_iota(jnp.int32, (1, 128), 1)
        lhs[...] = jnp.zeros_like(lhs)
        flat = parts.reshape(n_sp * 16, 128)
        for t in range(2):
            m = flat[pl.ds(t * 8 + 6, n_sp, stride=16), :]
            l = flat[pl.ds(t * 8 + 7, n_sp, stride=16), :]
            m_new, v_new = fresh[t]
            top = jnp.maximum(jnp.max(m, axis=0, keepdims=True), m_new)
            f = jnp.exp(m - top)
            f_new = jnp.exp(m_new - top)
            den = jnp.where(lane < 6, jnp.sum(f * l, axis=0, keepdims=True) + f_new, 1.0)
            wt = (jnp.concatenate([f, jnp.broadcast_to(f_new, (8, 128))], axis=0) / den).T
            sums = [wt[:8, n_sp:n_sp + 1] * v_new] + [jnp.zeros((8, 128), F32)] * 3
            for s in range(n_sp):
                sums[s % 4] += wt[:8, s:s + 1] * parts[s, t]
            acc = (sums[0] + sums[1]) + (sums[2] + sums[3])
            for hd in range(6):
                lhs[t:t + 1, hd * 128:(hd + 1) * 128] = acc[hd:hd + 1, :]

    me = group * 2 + tp
    with jax.named_scope("wout"):
        left = lhs[...].astype(BF16)
        for c in range(OWNERS):
            wo_copy(c).wait()
            res = jnp.dot(left, wo_buf[:, c * own:(c + 1) * own], preferred_element_type=F32)
            for t in range(2):
                for cb in range(n_cb):
                    mine[c, t, cb:cb + 1, :] = res[t:t + 1, cb * 128:(cb + 1) * 128]
                mine[c, t, n_cb:8, :] = jnp.zeros((8 - n_cb, 128), F32)

    with jax.named_scope("xsend"):
        for d in range(1, OWNERS):
            owner = lax.rem(me + d, OWNERS)
            pltpu.make_async_remote_copy(
                src_ref=mine.at[owner], dst_ref=shares.at[me], send_sem=x_send, recv_sem=x_recv,
                device_id={"tp": lax.rem(owner, 2), "sp": line * KV + lax.div(owner, 2)}, device_id_type=MESH).start()
        shares[me] = mine[me]
    x_others = shares.at[pl.ds(0, OWNERS - 1)]
    slot = group * n_lines + line
    with jax.named_scope("xwait"):
        pltpu.make_async_copy(x_others, x_others, x_recv).wait()
    with jax.named_scope("agsend"):
        total = shares[0]
        for s in range(1, OWNERS):
            total += shares[s]
        full[slot] = total

        def ag_start(d, carry):
            pltpu.make_async_remote_copy(
                src_ref=full.at[slot], dst_ref=full.at[slot], send_sem=ag_send, recv_sem=ag_recv,
                device_id={"sp": lax.rem(sp + d, n_sp)}, device_id_type=MESH).start()
            return carry

        lax.fori_loop(1, n_sp, ag_start, 0)
    f_others = full.at[pl.ds(0, n_sp - 1)]
    with jax.named_scope("agwait"):
        pltpu.make_async_copy(f_others, f_others, ag_recv).wait()
    swap = pltpu.make_async_remote_copy(
        src_ref=full, dst_ref=other, send_sem=tp_send, recv_sem=tp_recv, device_id={"tp": 1 - tp},
        device_id_type=MESH)
    swap.start()

    def finish(buf, core):
        buf = buf.reshape(n_sp * 16, 128)
        for g in range(KV):
            for cb in range(n_cb):
                slab = buf[pl.ds(g * n_lines * 16 + cb, n_seq, stride=8), :]
                at = pl.ds(pl.multiple_of((g * 2 + core) * own + cb * 128, 128), 128)
                out_ref[:, at] = (h_ref[:, at].astype(F32) + slab).astype(BF16)

    with jax.named_scope("finish1"):
        finish(full, tp)
    with jax.named_scope("swapwait"):
        swap.wait()
    with jax.named_scope("finish2"):
        finish(other, 1 - tp)
    with jax.named_scope("drain"):
        pltpu.make_async_copy(q_others, q_others, q_send).wait()
        pltpu.make_async_copy(others, others, rs_send).wait()
        pltpu.make_async_copy(x_others, x_others, x_send).wait()
        pltpu.make_async_copy(f_others, f_others, ag_send).wait()


def cache_kernel(pos_ref, new_ref, k_ref, v_ref, k_out, v_out, new_k, new_v, sem, row_sem):
    n_seq, seq_local = k_ref.shape[:2]
    base = lax.axis_index("sp") * seq_local
    copies = [pltpu.make_async_copy(k_ref, k_out, sem.at[0]), pltpu.make_async_copy(v_ref, v_out, sem.at[1])]
    for c in copies:
        c.start()
    for b in range(n_seq):
        tile = new_ref[b * 32:(b + 1) * 32, :].astype(F32)
        for buf, r in ((new_k, 6), (new_v, 7)):
            buf[b] = jnp.concatenate([tile[g * 8 + r:g * 8 + r + 1, :] for g in range(KV)], axis=0).astype(BF16)
    for c in copies:
        c.wait()

    def rows(b):
        at = pos_ref[b] - base
        return at, [pltpu.make_async_copy(new_k.at[b], k_out.at[b, at], row_sem),
                    pltpu.make_async_copy(new_v.at[b], v_out.at[b, at], row_sem)]

    for phase in range(2):
        for b in range(n_seq):
            at, pair = rows(b)

            @pl.when(jnp.logical_and(at >= 0, at < seq_local))
            def _():
                for c in pair:
                    if phase == 0:
                        c.start()
                    else:
                        c.wait()


def solution(mesh):
    cache_spec = P('dp', 'sp', 'tp', None)
    n_sp = mesh.shape["sp"]

    def local_step(hidden, norm_scale, w_qkv, w_out, k_cache, v_cache, positions):
        n_seq, seq_local, kv, head_dim = k_cache.shape
        d_model = hidden.shape[1]
        width = w_qkv.shape[1] // PLANE
        depth = w_out.shape[0] // kv
        vmem = pl.BlockSpec(memory_space=VMEM)
        smem = pl.BlockSpec(memory_space=pltpu.SMEM)
        hbm = pl.BlockSpec(memory_space=pltpu.HBM)
        half = head_dim // 2
        freq = np.exp(np.arange(half, dtype=np.float32) * np.float32(-2.0 * math.log(500000.0) / head_dim))
        freq = jnp.asarray(np.concatenate([freq, freq])[None].astype(np.float32))
        flat = (n_seq, seq_local * kv, head_dim)
        dma = pltpu.SemaphoreType.DMA

        h_out, new_rows = pl.pallas_call(
            step_kernel,
            out_shape=[jax.ShapeDtypeStruct((n_seq, d_model), BF16), jax.ShapeDtypeStruct((n_seq * 32, head_dim), BF16)],
            in_specs=[hbm] * 8,
            out_specs=[vmem, vmem],
            scratch_shapes=[
                pltpu.SMEM((n_seq,), jnp.int32),
                VMEM((n_seq, d_model), BF16),
                VMEM((d_model,), BF16),
                VMEM((1, head_dim), F32),
                dma((4,)),
                VMEM((d_model, width), BF16),
                VMEM((depth, d_model), BF16),
                VMEM(flat, BF16),
                VMEM(flat, BF16),
                VMEM((PLANE, n_seq, width), F32),
                VMEM((n_seq * 32, head_dim), F32),
                VMEM((n_seq * 32, head_dim), BF16),
                VMEM((n_seq // 2, kv, 2, 8, head_dim), F32),
                VMEM((n_sp, 2, 8, head_dim), F32),
                VMEM((8, depth), F32),
                VMEM((OWNERS, 2, 8, head_dim), F32),
                VMEM((OWNERS, 2, 8, head_dim), F32),
                VMEM((n_sp, 2, 8, head_dim), F32),
                VMEM((n_sp, 2, 8, head_dim), F32),
                dma((K_CHUNKS,)), dma((OWNERS,)), dma((2,)),
            ] + [dma] * 10,
            compiler_params=pltpu.CompilerParams(
                collective_id=0, has_side_effects=True, vmem_limit_bytes=32 * 1024 * 1024),
            cost_estimate=pl.CostEstimate(flops=60_000_000_000, bytes_accessed=20_000_000, transcendentals=0),
            name="step",
        )(*[pltpu.with_memory_space_constraint(a, pltpu.HBM) for a in (
            positions, hidden, norm_scale, freq, w_qkv, w_out, k_cache.reshape(flat), v_cache.reshape(flat))])

        k_new, v_new = pl.pallas_call(
            cache_kernel,
            out_shape=[jax.ShapeDtypeStruct(k_cache.shape, BF16)] * 2,
            in_specs=[smem, vmem, vmem, vmem],
            out_specs=[hbm, hbm],
            scratch_shapes=[VMEM((n_seq, kv, head_dim), BF16)] * 2 + [dma((2,)), dma],
            compiler_params=pltpu.CompilerParams(vmem_limit_bytes=16 * 1024 * 1024),
            name="cache",
        )(positions, new_rows, pltpu.with_memory_space_constraint(k_cache, VMEM),
          pltpu.with_memory_space_constraint(v_cache, VMEM))
        return h_out, k_new, v_new

    return jax.shard_map(
        local_step,
        mesh=mesh,
        in_specs=(P('dp', None), P(None), P(None, 'tp'), P('tp', None), cache_spec, cache_spec, P('dp')),
        out_specs=(P('dp', None), cache_spec, cache_spec),
        check_vma=False,
    )
```

```python
import itertools
import math

import jax
import jax.numpy as jnp
import numpy as np
from jax import lax
from jax.experimental import pallas as pl
from jax.experimental.pallas import tpu as pltpu
from jax.sharding import PartitionSpec as P

MESH = pl.DeviceIdType.MESH
VMEM = pltpu.VMEM
F32 = jnp.float32
BF16 = jnp.bfloat16
NEG = -3.0e38
PLANE = 16
K_CHUNKS = 6
KV = 4
OWNERS = 8
CHUNK = 4
RS_ROWS = 14
AG_ROWS = 12


def farthest_first(dims):
    near = lambda o: sum(min(v, 4 - v) for v in o)
    return sorted((o for o in itertools.product(range(4), repeat=dims) if any(o)), key=lambda o: -near(o))


PLANE_ORDER = farthest_first(2)
CUBE_ORDER = farthest_first(3)


def step_kernel(pos_hbm, h_hbm, scale_hbm, freq_hbm, wq_ref, wo_ref, k_ref, v_ref, out_ref, new_ref,
                pos_ref, h_ref, scale_ref, freq_ref, in_sem,
                wq_buf, wo_buf, k_buf, v_buf, recv, xs, xb, part, parts, lhs, mine, shares, full, other,
                wq_sem, wo_sem, kv_sem, q_send, q_recv, early_send, early_recv, late_send, late_recv,
                rs_send, rs_recv, x_send, x_recv, ag_send, ag_recv, tp_send, tp_recv):
    sp = lax.axis_index("sp")
    tp = lax.axis_index("tp")
    n_sp = 64
    line, group = lax.div(sp, KV), lax.rem(sp, KV)
    n_lines = n_sp // KV
    j = lax.rem(sp, PLANE)
    base = sp - j
    y_at, x_at = lax.div(j, 4), lax.rem(j, 4)
    is_kv = x_at == 3
    n_seq, d_model = h_ref.shape
    width = wq_buf.shape[1]
    heads_per = width // 128
    rows = d_model // K_CHUNKS
    n_rows = k_ref.shape[1]
    seq_local = n_rows // KV
    depth = wo_buf.shape[0]
    own = d_model // OWNERS
    n_cb = own // 128

    def wq_copy(c):
        return pltpu.make_async_copy(
            wq_ref.at[pl.ds(c * rows, rows), pl.ds(pl.multiple_of(j * width, width), width)],
            wq_buf.at[pl.ds(c * rows, rows)], wq_sem.at[c])

    wo_copy = pltpu.make_async_copy(wo_ref.at[pl.ds(pl.multiple_of(group * depth, depth), depth)], wo_buf, wo_sem)
    k_copy = pltpu.make_async_copy(k_ref, k_buf, kv_sem.at[0])
    v_copy = pltpu.make_async_copy(v_ref, v_buf, kv_sem.at[1])
    small = [pltpu.make_async_copy(src, dst, in_sem.at[i]) for i, (src, dst) in enumerate(
        [(h_hbm, h_ref), (pos_hbm, pos_ref), (freq_hbm, freq_ref), (scale_hbm, scale_ref)])]
    for c in small:
        c.start()
    for c in range(K_CHUNKS):
        wq_copy(c).start()

    barrier = pltpu.get_barrier_semaphore()

    def greet(d, carry):
        pl.semaphore_signal(barrier, inc=1, device_id={"sp": lax.rem(sp + d, n_sp)}, device_id_type=MESH)
        return carry

    with jax.named_scope("greet"):
        lax.fori_loop(1, n_sp, greet, 0)
        for d in range(KV):
            pl.semaphore_signal(barrier, inc=1, device_id={"tp": 1 - tp, "sp": line * KV + lax.rem(group + d, KV)},
                                device_id_type=MESH)

    with jax.named_scope("hwait"):
        small[0].wait()
    with jax.named_scope("norm"):
        hidden = h_ref[...].astype(F32)
        centered = hidden - jnp.mean(hidden, axis=-1, keepdims=True)
        var = jnp.mean(centered * centered, axis=-1, keepdims=True)
    with jax.named_scope("inwait"):
        for c in small[1:]:
            c.wait()
        k_copy.start()
        v_copy.start()
    with jax.named_scope("norm2"):
        u = (centered * lax.rsqrt(var + 1e-5) * scale_ref[...].astype(F32)[None, :]).astype(BF16)
        seq_row = lax.broadcasted_iota(jnp.int32, (n_seq, 128), 0)
        pos = jnp.zeros((n_seq, 128), jnp.int32)
        for b in range(n_seq):
            pos = jnp.where(seq_row == b, pos_ref[b], pos)
        angles = pos.astype(F32) * freq_ref[...]
        cos = jnp.cos(angles)
        sin = jnp.sin(angles)
        sin = jnp.where(lax.broadcasted_iota(jnp.int32, (n_seq, 128), 1) < 64, -sin, sin)

    with jax.named_scope("qkv"):
        acc = jnp.zeros((n_seq, width), F32)
        for c in range(K_CHUNKS):
            wq_copy(c).wait()
            acc += jnp.dot(u[:, c * rows:(c + 1) * rows], wq_buf[c * rows:(c + 1) * rows, :],
                           preferred_element_type=F32)
        y = jnp.clip(acc.astype(BF16), -8.0, 8.0).astype(F32)
        heads = []
        for i in range(heads_per):
            piece = y[:, i * 128:(i + 1) * 128]
            turned = (piece * cos + pltpu.roll(piece, 64, 1) * sin).astype(BF16).astype(F32)
            heads.append(turned if i == 0 else jnp.where(is_kv, piece, turned))
        recv[j] = jnp.concatenate(heads, axis=1)
        wo_copy.start()
    with jax.named_scope("barrier"):
        pl.semaphore_wait(barrier, n_sp - 1 + KV)

    def to_plane(dy, dx, send_sem, recv_sem):
        peer = base + lax.rem(y_at + dy, 4) * 4 + lax.rem(x_at + dx, 4)
        return pltpu.make_async_remote_copy(
            src_ref=recv.at[j], dst_ref=recv.at[j], send_sem=send_sem, recv_sem=recv_sem,
            device_id={"sp": peer}, device_id_type=MESH)

    def blocks(n):
        return recv.at[pl.ds(0, n)]

    def wait_for(n, sem):
        pltpu.make_async_copy(blocks(n), blocks(n), sem).wait()

    is_last = jnp.logical_and(is_kv, y_at == 3)
    with jax.named_scope("qsend"):
        @pl.when(jnp.logical_not(is_kv))
        def _():
            for dy, dx in PLANE_ORDER:
                to_plane(dy, dx, q_send, q_recv).start()

        @pl.when(is_kv)
        def _():
            for dy in (2, 1, 3, 0):
                @pl.when(jnp.logical_or(dy != 0, y_at != 3))
                def _():
                    to_plane(dy, lax.rem(y_at + 1, 4), early_send, early_recv).start()

        for g in range(KV):
            for r in (6, 7):
                xs[pl.ds(g * 8 + r, n_seq, stride=32), :] = jnp.zeros((n_seq, 128), F32)
    with jax.named_scope("qwait"):
        @pl.when(is_kv)
        def _():
            wait_for(12, q_recv)

        @pl.when(jnp.logical_not(is_kv))
        def _():
            wait_for(11, q_recv)
    with jax.named_scope("spread"):
        for blk in range(PLANE):
            if blk % 4 == 3:
                continue
            for i in range(heads_per):
                xs[pl.ds(blk * heads_per + i, n_seq, stride=32), :] = recv[blk, :, i * 128:(i + 1) * 128]
        xb[...] = xs[...].astype(BF16)

    row8 = lax.broadcasted_iota(jnp.int32, (32, 128), 0) % 8
    lane32 = lax.broadcasted_iota(jnp.int32, (32, 128), 1)

    def as_rows(cols, n):
        tiles = sum(jnp.where((lane32 == row8 + 8 * t)[:8 * n], c, 0.0) for t, c in enumerate(cols)).reshape(n, 8, 128)
        return jnp.broadcast_to(jnp.sum(tiles, axis=1, keepdims=True), (n, 8, 128)).reshape(8 * n, 128)

    with jax.named_scope("kvwait"):
        k_copy.wait()
        v_copy.wait()
    row = lax.broadcasted_iota(jnp.int32, (32, n_rows), 0)
    col = lax.broadcasted_iota(jnp.int32, (32, n_rows), 1)
    seq_of = jnp.where(col % KV == row // 8, col // KV + sp * seq_local, 1 << 30)
    scale = 128 ** -0.5

    def line_at(i):
        return lax.rem(line + 1 + i, n_lines)

    def scores(c):
        out = []
        for i in range(CHUNK):
            for t in range(2):
                b = line_at(c * CHUNK + i) + 16 * t
                q = xb[pl.ds(pl.multiple_of(b * 32, 32), 32), :]
                s = lax.dot_general(q, k_buf[b], (((1,), (1,)), ((), ())), preferred_element_type=F32) * scale
                out.append(jnp.where(seq_of < pos_ref[b], s, NEG))
        return out

    with jax.named_scope("attn"):
        n_chunks = n_lines // CHUNK
        held = scores(0)
        for c in range(n_chunks):
            ahead = scores(c + 1) if c + 1 < n_chunks else None
            for i in range(CHUNK):
                ln = line_at(c * CHUNK + i)
                stats, outs = [], []
                for t in range(2):
                    s = held[i * 2 + t]
                    m = jnp.max(s, axis=1, keepdims=True)
                    e = jnp.exp(s - m)
                    stats.append((m, jnp.sum(e, axis=1, keepdims=True)))
                    outs.append(jnp.dot(e.astype(BF16), v_buf[ln + 16 * t], preferred_element_type=F32))
                (m0, l0), (m1, l1) = stats
                first = jnp.where(row8 == 6, as_rows((m0, m1), KV), jnp.where(row8 == 7, as_rows((l0, l1), KV), outs[0]))
                for g in range(KV):
                    at = pl.multiple_of((ln * KV + g) * 16, 16)
                    part[pl.ds(at, 8), :] = first[g * 8:(g + 1) * 8]
                    part[pl.ds(at + 8, 8), :] = outs[1][g * 8:(g + 1) * 8]
            for i in range(CHUNK):
                ln = line_at(c * CHUNK + i)
                for d in (2, 1, 3, 0):
                    if c * CHUNK + i == n_lines - 1 and d == 0:
                        continue
                    to = lax.rem(group + d, KV)
                    pltpu.make_async_remote_copy(
                        src_ref=part.at[pl.ds(pl.multiple_of((ln * KV + to) * 16, 16), RS_ROWS)],
                        dst_ref=parts.at[pl.ds(pl.multiple_of(sp * 16, 16), RS_ROWS)], send_sem=rs_send,
                        recv_sem=rs_recv, device_id={"sp": ln * KV + to}, device_id_type=MESH).start()
            held = ahead
        parts[pl.ds(pl.multiple_of(sp * 16, 16), 16), :] = part[pl.ds(pl.multiple_of(sp * 16, 16), 16), :]

    with jax.named_scope("newrow"):
        @pl.when(jnp.logical_not(is_last))
        def _():
            wait_for(1, early_recv)

        for i in range(heads_per):
            xs[pl.ds(group * 8 + 6 + i, n_seq, stride=32), :] = recv[group * 4 + 3, :, i * 128:(i + 1) * 128]
        cols, v_new = [], []
        for t in range(2):
            tile = xs[pl.ds(pl.multiple_of((line + 16 * t) * 32 + group * 8, 8), 8), :]
            cols.append(jnp.sum(tile * tile[6:7, :], axis=1, keepdims=True) * scale)
            v_new.append(tile[7:8, :])
        m_new = as_rows(cols, 1)[:1]

    rs_others = parts.at[pl.ds(0, (n_sp - 1) * RS_ROWS)]
    with jax.named_scope("rswait"):
        pltpu.make_async_copy(rs_others, rs_others, rs_recv).wait()

    with jax.named_scope("latesend"):
        @pl.when(is_kv)
        def _():
            for dx in (1, 2, 3, 4):
                for dy in (0, 1, 2, 3):
                    to_x = lax.rem(x_at + dx, 4)
                    ok = to_x != y_at
                    if dx == 4 and dy == 0:
                        continue

                    @pl.when(ok)
                    def _():
                        to_plane(dy, dx, late_send, late_recv).start()

    with jax.named_scope("merge"):
        lane = lax.broadcasted_iota(jnp.int32, (1, 128), 1)
        m = parts[pl.ds(6, n_sp, stride=16), :]
        l = parts[pl.ds(7, n_sp, stride=16), :]
        top = jnp.maximum(jnp.max(m, axis=0, keepdims=True), m_new)
        f = jnp.exp(m - top)
        f_new = jnp.exp(m_new - top)
        real = jnp.logical_and(lane < 16, lane % 8 < 6)
        den = jnp.where(real, jnp.sum(f * l, axis=0, keepdims=True) + f_new, 1.0)
        wt = (jnp.concatenate([f, jnp.broadcast_to(f_new, (8, 128))], axis=0) / den).T
        lhs[...] = jnp.zeros_like(lhs)
        for t in range(2):
            w8 = wt[t * 8:(t + 1) * 8]
            sums = [w8[:, n_sp:n_sp + 1] * v_new[t]] + [jnp.zeros((8, 128), F32)] * 3
            for s in range(n_sp):
                sums[s % 4] += w8[:, s:s + 1] * parts[s * 16 + t * 8:s * 16 + t * 8 + 8, :]
            acc = (sums[0] + sums[1]) + (sums[2] + sums[3])
            for hd in range(6):
                lhs[t:t + 1, hd * 128:(hd + 1) * 128] = acc[hd:hd + 1, :]

    me = group * 2 + tp
    with jax.named_scope("wowait"):
        wo_copy.wait()
    with jax.named_scope("wout"):
        left = lhs[...].astype(BF16)
        order = [(dg, dt) for dg in (2, 1, 3, 0) for dt in (1, 0)]

        def product(k):
            owner = lax.rem(group + order[k][0], KV) * 2 + (tp if order[k][1] == 0 else 1 - tp)
            at = pl.multiple_of(owner * own, own)
            return owner, jnp.dot(left, wo_buf[:, pl.ds(at, own)], preferred_element_type=F32)

        held = product(0)
        for k in range(OWNERS):
            ahead = product(k + 1) if k + 1 < OWNERS else None
            owner, res = held
            buf = mine if k < OWNERS - 1 else shares
            at = pl.multiple_of(owner * 16, 16)
            for t in range(2):
                for cb in range(n_cb):
                    buf[pl.ds(at + t * n_cb + cb, 1), :] = res[t:t + 1, cb * 128:(cb + 1) * 128]
            if k < OWNERS - 1:
                pltpu.make_async_remote_copy(
                    src_ref=mine.at[pl.ds(at, AG_ROWS)],
                    dst_ref=shares.at[pl.ds(pl.multiple_of(me * 16, 16), AG_ROWS)], send_sem=x_send, recv_sem=x_recv,
                    device_id={"tp": lax.rem(owner, 2), "sp": line * KV + lax.div(owner, 2)},
                    device_id_type=MESH).start()
            held = ahead

    x_others = shares.at[pl.ds(0, (OWNERS - 1) * AG_ROWS)]
    slot = group * n_lines + line
    with jax.named_scope("xwait"):
        pltpu.make_async_copy(x_others, x_others, x_recv).wait()
    z_at = lax.div(sp, PLANE)
    with jax.named_scope("agsend"):
        total = shares[0:16, :]
        for s in range(1, OWNERS):
            total += shares[s * 16:(s + 1) * 16, :]
        at = pl.multiple_of(slot * 16, 16)
        full[pl.ds(at, 16), :] = total
        zs = [lax.rem(z_at + d, 4) * 16 for d in range(4)]
        ys = [lax.rem(y_at + d, 4) * 4 for d in range(4)]
        xs_ = [lax.rem(x_at + d, 4) for d in range(4)]
        for dz, dy, dx in CUBE_ORDER:
            pltpu.make_async_remote_copy(
                src_ref=full.at[pl.ds(at, AG_ROWS)], dst_ref=full.at[pl.ds(at, AG_ROWS)], send_sem=ag_send,
                recv_sem=ag_recv.at[group], device_id={"sp": zs[dz] + ys[dy] + xs_[dx]}, device_id_type=MESH).start()

    def finish(buf, g, core):
        for cb in range(n_cb):
            at = pl.ds(pl.multiple_of((g * 2 + core) * own + cb * 128, 128), 128)
            for t in range(2):
                slab = buf[pl.ds(g * n_lines * 16 + t * n_cb + cb, n_lines, stride=16), :]
                out_ref[t * 16:(t + 1) * 16, at] = (h_ref[t * 16:(t + 1) * 16, at].astype(F32) + slab).astype(BF16)

    def quarter(k):
        g = lax.rem(group + k, KV)
        at = pl.ds(pl.multiple_of(g * n_lines * 16, 256), n_lines * 16)
        return g, pltpu.make_async_remote_copy(
            src_ref=full.at[at], dst_ref=other.at[at], send_sem=tp_send.at[k], recv_sem=tp_recv.at[g],
            device_id={"tp": 1 - tp}, device_id_type=MESH)

    with jax.named_scope("agwait"):
        for k in (0, 1, 3, 2):
            g, swap = quarter(k)
            n = (n_lines if k else n_lines - 1) * AG_ROWS
            pltpu.make_async_copy(full.at[pl.ds(0, n)], full.at[pl.ds(0, n)], ag_recv.at[g]).wait()
            swap.start()
            finish(full, g, tp)
    with jax.named_scope("swapwait"):
        for k in (0, 1, 3, 2):
            g, swap = quarter(k)
            swap.wait()
            finish(other, g, 1 - tp)
    with jax.named_scope("drain"):
        @pl.when(jnp.logical_and(is_kv, jnp.logical_not(is_last)))
        def _():
            wait_for(2, late_recv)
            wait_for(4, early_send)
            wait_for(11, late_send)

        @pl.when(is_last)
        def _():
            wait_for(3, late_recv)
            wait_for(3, early_send)
            wait_for(12, late_send)

        @pl.when(jnp.logical_not(is_kv))
        def _():
            wait_for(3, late_recv)
            wait_for(PLANE - 1, q_send)

        for g in range(KV):
            for i in range(heads_per):
                at = (i * KV + g) * n_seq
                new_ref[at:at + n_seq, :] = recv[g * 4 + 3, :, i * 128:(i + 1) * 128]
        pltpu.make_async_copy(rs_others, rs_others, rs_send).wait()
        pltpu.make_async_copy(x_others, x_others, x_send).wait()
        f_others = full.at[pl.ds(0, (n_sp - 1) * AG_ROWS)]
        pltpu.make_async_copy(f_others, f_others, ag_send).wait()


def cache_kernel(pos_ref, new_ref, k_ref, v_ref, h_ref, k_out, v_out, h_out, k_fix, v_fix, sem):
    n_seq, seq_local = k_ref.shape[:2]
    base = lax.axis_index("sp") * seq_local
    trio = ((k_ref, k_fix, k_out), (v_ref, v_fix, v_out))
    hidden = pltpu.make_async_copy(h_ref, h_out, sem.at[2])
    hidden.start()
    for b in range(n_seq):
        at = pos_ref[b] - base
        here = jnp.logical_and(at >= 0, at < seq_local)

        @pl.when(jnp.logical_not(here))
        def _():
            for i, (src, _, dst) in enumerate(trio):
                pltpu.make_async_copy(src.at[b], dst.at[b], sem.at[i]).start()

        @pl.when(here)
        def _():
            for i, (src, fix, dst) in enumerate(trio):
                fix[b] = src[b]
                fix[b, at] = new_ref[pl.ds(i * KV * n_seq + b, KV, stride=n_seq), :].astype(BF16)
                pltpu.make_async_copy(fix.at[b], dst.at[b], sem.at[i]).start()

    for i, (src, _, dst) in enumerate(trio):
        pltpu.make_async_copy(src, dst, sem.at[i]).wait()
    hidden.wait()


def solution(mesh):
    cache_spec = P('dp', 'sp', 'tp', None)
    n_sp = mesh.shape["sp"]

    def local_step(hidden, norm_scale, w_qkv, w_out, k_cache, v_cache, positions):
        n_seq, seq_local, kv, head_dim = k_cache.shape
        d_model = hidden.shape[1]
        width = w_qkv.shape[1] // PLANE
        depth = w_out.shape[0] // kv
        vmem = pl.BlockSpec(memory_space=VMEM)
        smem = pl.BlockSpec(memory_space=pltpu.SMEM)
        hbm = pl.BlockSpec(memory_space=pltpu.HBM)
        half = head_dim // 2
        freq = np.exp(np.arange(half, dtype=np.float32) * np.float32(-2.0 * math.log(500000.0) / head_dim))
        freq = jnp.asarray(np.concatenate([freq, freq])[None].astype(np.float32))
        flat = (n_seq, seq_local * kv, head_dim)
        dma = pltpu.SemaphoreType.DMA

        h_new, new_rows = pl.pallas_call(
            step_kernel,
            out_shape=[jax.ShapeDtypeStruct((n_seq, d_model), BF16), jax.ShapeDtypeStruct((2 * kv * n_seq, head_dim), F32)],
            in_specs=[hbm] * 8,
            out_specs=[vmem, vmem],
            scratch_shapes=[
                pltpu.SMEM((n_seq,), jnp.int32),
                VMEM((n_seq, d_model), BF16),
                VMEM((d_model,), BF16),
                VMEM((1, head_dim), F32),
                dma((4,)),
                VMEM((d_model, width), BF16),
                VMEM((depth, d_model), BF16),
                VMEM(flat, BF16),
                VMEM(flat, BF16),
                VMEM((PLANE, n_seq, width), F32),
                VMEM((n_seq * 32, head_dim), F32),
                VMEM((n_seq * 32, head_dim), BF16),
                VMEM((n_sp * 16, head_dim), F32),
                VMEM((n_sp * 16, head_dim), F32),
                VMEM((8, depth), F32),
                VMEM((OWNERS * 16, head_dim), F32),
                VMEM((OWNERS * 16, head_dim), F32),
                VMEM((n_sp * 16, head_dim), F32),
                VMEM((n_sp * 16, head_dim), F32),
                dma((K_CHUNKS,)), dma, dma((2,)),
            ] + [dma] * 11 + [dma((kv,))] * 3,
            compiler_params=pltpu.CompilerParams(
                collective_id=0, has_side_effects=True, vmem_limit_bytes=32 * 1024 * 1024),
            cost_estimate=pl.CostEstimate(flops=60_000_000_000, bytes_accessed=20_000_000, transcendentals=0),
            name="step",
        )(*[pltpu.with_memory_space_constraint(a, pltpu.HBM) for a in (
            positions, hidden, norm_scale, freq, w_qkv, w_out, k_cache.reshape(flat), v_cache.reshape(flat))])

        k_new, v_new, h_out = pl.pallas_call(
            cache_kernel,
            out_shape=[jax.ShapeDtypeStruct(k_cache.shape, BF16)] * 2 + [jax.ShapeDtypeStruct((n_seq, d_model), BF16)],
            in_specs=[smem, vmem, vmem, vmem, vmem],
            out_specs=[hbm, hbm, hbm],
            scratch_shapes=[VMEM(k_cache.shape, BF16)] * 2 + [dma((3,))],
            compiler_params=pltpu.CompilerParams(vmem_limit_bytes=16 * 1024 * 1024),
            name="cache",
        )(positions, new_rows, pltpu.with_memory_space_constraint(k_cache, VMEM),
          pltpu.with_memory_space_constraint(v_cache, VMEM), h_new)
        return h_out, k_new, v_new

    return jax.shard_map(
        local_step,
        mesh=mesh,
        in_specs=(P('dp', None), P(None), P(None, 'tp'), P('tp', None), cache_spec, cache_spec, P('dp')),
        out_specs=(P('dp', None), cache_spec, cache_spec),
        check_vma=False,
    )
```

```python
import itertools
import math

import jax
import jax.numpy as jnp
import numpy as np
from jax import lax
from jax.experimental import pallas as pl
from jax.experimental.pallas import tpu as pltpu
from jax.sharding import PartitionSpec as P

MESH = pl.DeviceIdType.MESH
VMEM = pltpu.VMEM
F32 = jnp.float32
BF16 = jnp.bfloat16
NEG = -3.0e38
PLANE = 16
K_CHUNKS = 6
KV = 4
OWNERS = 8
TURNS = (2, 1, 3, 0)
QUARTERS = (0, 1, 3, 2)
RS_ROWS = 14
AG_ROWS = 12


def farthest_first(dims):
    near = lambda o: sum(min(v, 4 - v) for v in o)
    return sorted((o for o in itertools.product(range(4), repeat=dims) if any(o)), key=lambda o: -near(o))


PLANE_ORDER = farthest_first(2)
CUBE_ORDER = farthest_first(3)


def step_kernel(pos_hbm, h_hbm, scale_hbm, freq_hbm, wq_ref, wo_ref, k_ref, v_ref, out_ref, new_ref,
                pos_ref, h_ref, scale_ref, freq_ref, in_sem,
                wq_buf, wo_buf, k_buf, v_buf, recv, xs, xb, part, parts, full, prods, other,
                wq_sem, wo_sem, kv_sem, q_send, q_recv, early_send, early_recv, late_send, late_recv,
                rs_send, rs_recv, ag_send, ag_recv, tp_send, tp_recv, ready):
    sp = lax.axis_index("sp")
    tp = lax.axis_index("tp")
    n_sp = 64
    line, group = lax.div(sp, KV), lax.rem(sp, KV)
    n_lines = n_sp // KV
    j = lax.rem(sp, PLANE)
    base = sp - j
    y_at, x_at = lax.div(j, 4), lax.rem(j, 4)
    z_at = lax.div(sp, PLANE)
    is_kv = x_at == 3
    n_seq, d_model = h_ref.shape
    width = wq_buf.shape[1]
    heads_per = width // 128
    rows = d_model // K_CHUNKS
    n_rows = k_ref.shape[1]
    seq_local = n_rows // KV
    depth = wo_buf.shape[1]
    own = d_model // OWNERS

    def turn_of(dz):
        return jnp.where(dz == 2, 0, jnp.where(dz == 1, 1, jnp.where(dz == 3, 2, 3)))

    def wq_copy(c):
        return pltpu.make_async_copy(
            wq_ref.at[pl.ds(c * rows, rows), pl.ds(pl.multiple_of(j * width, width), width)],
            wq_buf.at[pl.ds(c * rows, rows)], wq_sem.at[c])

    def wo_copy(k):
        g = lax.rem(group + 4 - QUARTERS[k], KV)
        return pltpu.make_async_copy(wo_ref.at[pl.ds(pl.multiple_of(g * depth, depth), depth)], wo_buf.at[g], wo_sem.at[k])

    k_copy = pltpu.make_async_copy(k_ref, k_buf, kv_sem.at[0])
    v_copy = pltpu.make_async_copy(v_ref, v_buf, kv_sem.at[1])
    small = [pltpu.make_async_copy(src, dst, in_sem.at[i]) for i, (src, dst) in enumerate(
        [(h_hbm, h_ref), (pos_hbm, pos_ref), (freq_hbm, freq_ref), (scale_hbm, scale_ref)])]
    for c in small:
        c.start()
    for c in range(K_CHUNKS):
        wq_copy(c).start()

    barrier = pltpu.get_barrier_semaphore()

    with jax.named_scope("greet"):
        for dy, dx in PLANE_ORDER:
            peer = base + lax.rem(y_at + dy, 4) * 4 + lax.rem(x_at + dx, 4)
            pl.semaphore_signal(barrier, inc=1, device_id={"sp": peer}, device_id_type=MESH)
        for dz in range(1, 4):
            pl.semaphore_signal(barrier, inc=1, device_id={"sp": lax.rem(sp + dz * PLANE, n_sp)}, device_id_type=MESH)
        pl.semaphore_signal(barrier, inc=1, device_id={"tp": 1 - tp}, device_id_type=MESH)

    with jax.named_scope("hwait"):
        small[0].wait()
    with jax.named_scope("norm"):
        hidden = h_ref[...].astype(F32)
        centered = hidden - jnp.mean(hidden, axis=-1, keepdims=True)
        var = jnp.mean(centered * centered, axis=-1, keepdims=True)
    with jax.named_scope("inwait"):
        for c in small[1:]:
            c.wait()
        k_copy.start()
        v_copy.start()
    with jax.named_scope("norm2"):
        u = (centered * lax.rsqrt(var + 1e-5) * scale_ref[...].astype(F32)[None, :]).astype(BF16)
        seq_row = lax.broadcasted_iota(jnp.int32, (n_seq, 128), 0)
        pos = jnp.zeros((n_seq, 128), jnp.int32)
        for b in range(n_seq):
            pos = jnp.where(seq_row == b, pos_ref[b], pos)
        angles = pos.astype(F32) * freq_ref[...]
        cos = jnp.cos(angles)
        sin = jnp.sin(angles)
        sin = jnp.where(lax.broadcasted_iota(jnp.int32, (n_seq, 128), 1) < 64, -sin, sin)

    with jax.named_scope("qkv"):
        acc = jnp.zeros((n_seq, width), F32)
        for c in range(K_CHUNKS):
            wq_copy(c).wait()
            acc += jnp.dot(u[:, c * rows:(c + 1) * rows], wq_buf[c * rows:(c + 1) * rows, :],
                           preferred_element_type=F32)
        y = jnp.clip(acc.astype(BF16), -8.0, 8.0).astype(F32)
        heads = []
        for i in range(heads_per):
            piece = y[:, i * 128:(i + 1) * 128]
            turned = (piece * cos + pltpu.roll(piece, 64, 1) * sin).astype(BF16).astype(F32)
            heads.append(turned if i == 0 else jnp.where(is_kv, piece, turned))
        y = jnp.concatenate(heads, axis=1)
        for z in range(4):
            tile = jnp.concatenate([y[z * 4:z * 4 + 4], y[16 + z * 4:16 + z * 4 + 4]], axis=0)
            recv[j, turn_of(lax.rem(z + 4 - z_at, 4))] = tile
        for k in range(KV):
            wo_copy(k).start()
    with jax.named_scope("barrier"):
        pl.semaphore_wait(barrier, PLANE - 1 + 3 + 1)

    def to_plane(dy, dx, send_sem, recv_sem, tiles=pl.ds(0, 4)):
        peer = base + lax.rem(y_at + dy, 4) * 4 + lax.rem(x_at + dx, 4)
        return pltpu.make_async_remote_copy(
            src_ref=recv.at[j, tiles], dst_ref=recv.at[j, tiles], send_sem=send_sem, recv_sem=recv_sem,
            device_id={"sp": peer}, device_id_type=MESH)

    def blocks(n):
        return recv.at[pl.ds(0, n)]

    def wait_for(n, sem):
        pltpu.make_async_copy(blocks(n), blocks(n), sem).wait()

    def wait_for_halves(n, sem):
        flat_half = xs.at[pl.ds(0, n * n_seq * width // 256)]
        pltpu.make_async_copy(flat_half, flat_half, sem).wait()

    is_last = jnp.logical_and(is_kv, y_at == 3)
    with jax.named_scope("qsend"):
        @pl.when(jnp.logical_not(is_kv))
        def _():
            for half in range(2):
                for dy, dx in PLANE_ORDER:
                    to_plane(dy, dx, q_send, q_recv.at[half], pl.ds(half * 2, 2)).start()

        @pl.when(is_kv)
        def _():
            for dy in (2, 1, 3, 0):
                @pl.when(jnp.logical_or(dy != 0, y_at != 3))
                def _():
                    to_plane(dy, lax.rem(y_at + 1, 4), early_send, early_recv).start()

        for dz in range(1, 4):
            pl.semaphore_signal(ready, inc=1, device_id={"sp": lax.rem(sp + dz * PLANE, n_sp)}, device_id_type=MESH)
        for g in range(KV):
            for r in (6, 7):
                xs[pl.ds(g * 8 + r, n_seq, stride=32), :] = jnp.zeros((n_seq, 128), F32)

    def half_queries(half):
        with jax.named_scope(f"qwait{half}"):
            @pl.when(is_kv)
            def _():
                wait_for_halves(12, q_recv.at[half])

            @pl.when(jnp.logical_not(is_kv))
            def _():
                wait_for_halves(11, q_recv.at[half])
        with jax.named_scope("spread"):
            for turn in (half * 2, half * 2 + 1):
                for blk in range(PLANE):
                    if blk % 4 == 3:
                        continue
                    for i in range(heads_per):
                        xs[pl.ds(turn * 256 + blk * heads_per + i, 8, stride=32), :] = (
                            recv[blk, turn, :, i * 128:(i + 1) * 128])
                xb[turn * 256:(turn + 1) * 256, :] = xs[turn * 256:(turn + 1) * 256, :].astype(BF16)

    row8 = lax.broadcasted_iota(jnp.int32, (32, 128), 0) % 8
    lane32 = lax.broadcasted_iota(jnp.int32, (32, 128), 1)

    def as_rows(cols, n):
        tiles = sum(jnp.where((lane32 == row8 + 8 * t)[:8 * n], c, 0.0) for t, c in enumerate(cols)).reshape(n, 8, 128)
        return jnp.broadcast_to(jnp.sum(tiles, axis=1, keepdims=True), (n, 8, 128)).reshape(8 * n, 128)

    with jax.named_scope("kvwait"):
        k_copy.wait()
        v_copy.wait()
    row = lax.broadcasted_iota(jnp.int32, (32, n_rows), 0)
    col = lax.broadcasted_iota(jnp.int32, (32, n_rows), 1)
    seq_of = jnp.where(col % KV == row // 8, col // KV + sp * seq_local, 1 << 30)
    scale = 128 ** -0.5

    def line_at(turn, i):
        return lax.rem(z_at + TURNS[turn], 4) * 4 + lax.rem(y_at + TURNS[i], 4)

    def scores(turn):
        out = []
        for i in range(4):
            for t in range(2):
                at = (turn * 8 + t * 4 + lax.rem(y_at + TURNS[i], 4)) * 32
                b = line_at(turn, i) + 16 * t
                q = xb[pl.ds(pl.multiple_of(at, 32), 32), :]
                s = lax.dot_general(q, k_buf[b], (((1,), (1,)), ((), ())), preferred_element_type=F32) * scale
                out.append(jnp.where(seq_of < pos_ref[b], s, NEG))
        return out

    def values(turn, held):
        for i in range(4):
            ln = line_at(turn, i)
            stats, outs = [], []
            for t in range(2):
                s = held[i * 2 + t]
                m = jnp.max(s, axis=1, keepdims=True)
                e = jnp.exp(s - m)
                stats.append((m, jnp.sum(e, axis=1, keepdims=True)))
                outs.append(jnp.dot(e.astype(BF16), v_buf[ln + 16 * t], preferred_element_type=F32))
            (m0, l0), (m1, l1) = stats
            first = jnp.where(row8 == 6, as_rows((m0, m1), KV), jnp.where(row8 == 7, as_rows((l0, l1), KV), outs[0]))
            for g in range(KV):
                at = pl.multiple_of((ln * KV + g) * 16, 16)
                part[pl.ds(at, 8), :] = first[g * 8:(g + 1) * 8]
                part[pl.ds(at + 8, 8), :] = outs[1][g * 8:(g + 1) * 8]

    def send_partials(turn):
        for i in range(4):
            ln = line_at(turn, i)
            for d in TURNS:
                if turn == 3 and i == 3 and d == 0:
                    continue
                to = lax.rem(group + d, KV)
                pltpu.make_async_remote_copy(
                    src_ref=part.at[pl.ds(pl.multiple_of((ln * KV + to) * 16, 16), RS_ROWS)],
                    dst_ref=parts.at[pl.ds(pl.multiple_of(sp * 16, 16), RS_ROWS)], send_sem=rs_send,
                    recv_sem=rs_recv, device_id={"sp": ln * KV + to}, device_id_type=MESH).start()

    half_queries(0)
    with jax.named_scope("ready"):
        pl.semaphore_wait(ready, 3)
    with jax.named_scope("attn0"):
        held = scores(0)
        ahead = scores(1)
        values(0, held)
        send_partials(0)
        values(1, ahead)
        send_partials(1)
    half_queries(1)
    with jax.named_scope("attn1"):
        held = scores(2)
        ahead = scores(3)
        values(2, held)
        send_partials(2)
        values(3, ahead)
        send_partials(3)
        parts[pl.ds(pl.multiple_of(sp * 16, 16), 16), :] = part[pl.ds(pl.multiple_of(sp * 16, 16), 16), :]

    with jax.named_scope("newrow"):
        @pl.when(jnp.logical_not(is_last))
        def _():
            wait_for(1, early_recv)

        for i in range(heads_per):
            xs[pl.ds(3 * 256 + group * 8 + 6 + i, 8, stride=32), :] = recv[group * 4 + 3, 3, :, i * 128:(i + 1) * 128]
        cols, v_new = [], []
        for t in range(2):
            tile = xs[pl.ds(pl.multiple_of((24 + t * 4 + y_at) * 32 + group * 8, 8), 8), :]
            cols.append(jnp.sum(tile * tile[6:7, :], axis=1, keepdims=True) * scale)
            v_new.append(tile[7:8, :])
        m_new = as_rows(cols, 1)[:1]

    rs_others = parts.at[pl.ds(0, (n_sp - 1) * RS_ROWS)]
    with jax.named_scope("rswait"):
        pltpu.make_async_copy(rs_others, rs_others, rs_recv).wait()

    with jax.named_scope("latesend"):
        @pl.when(is_kv)
        def _():
            for dx in (1, 2, 3, 4):
                for dy in (0, 1, 2, 3):
                    to_x = lax.rem(x_at + dx, 4)
                    ok = to_x != y_at
                    if dx == 4 and dy == 0:
                        continue

                    @pl.when(ok)
                    def _():
                        to_plane(dy, dx, late_send, late_recv).start()

    with jax.named_scope("merge"):
        lane = lax.broadcasted_iota(jnp.int32, (1, 128), 1)
        m = parts[pl.ds(6, n_sp, stride=16), :]
        l = parts[pl.ds(7, n_sp, stride=16), :]
        top = jnp.maximum(jnp.max(m, axis=0, keepdims=True), m_new)
        f = jnp.exp(m - top)
        f_new = jnp.exp(m_new - top)
        real = jnp.logical_and(lane < 16, lane % 8 < 6)
        den = jnp.where(real, jnp.sum(f * l, axis=0, keepdims=True) + f_new, 1.0)
        wt = (jnp.concatenate([f, jnp.broadcast_to(f_new, (8, 128))], axis=0) / den).T
        slot = pl.multiple_of((group * n_lines + line) * 16, 16)
        for t in range(2):
            w8 = wt[t * 8:(t + 1) * 8]
            sums = [w8[:, n_sp:n_sp + 1] * v_new[t]] + [jnp.zeros((8, 128), F32)] * 3
            for s in range(n_sp):
                sums[s % 4] += w8[:, s:s + 1] * parts[s * 16 + t * 8:s * 16 + t * 8 + 8, :]
            acc = ((sums[0] + sums[1]) + (sums[2] + sums[3])).astype(BF16).astype(F32)
            for hd in range(6):
                full[pl.ds(slot + t * 6 + hd, 1), :] = acc[hd:hd + 1, :]

    with jax.named_scope("agsend"):
        mine_rows = full.at[pl.ds(slot, AG_ROWS)]
        zs = [lax.rem(z_at + d, 4) * 16 for d in range(4)]
        ys = [lax.rem(y_at + d, 4) * 4 for d in range(4)]
        xs_ = [lax.rem(x_at + d, 4) for d in range(4)]
        for dx in QUARTERS:
            for dz, dy in [(0, 0)] * (dx > 0) + PLANE_ORDER[::-1]:
                pltpu.make_async_remote_copy(
                    src_ref=mine_rows, dst_ref=mine_rows, send_sem=ag_send, recv_sem=ag_recv.at[group],
                    device_id={"sp": zs[dz] + ys[dy] + xs_[dx]}, device_id_type=MESH).start()

    def swap(n):
        return pltpu.make_async_remote_copy(
            src_ref=prods.at[0, n], dst_ref=other.at[n], send_sem=tp_send.at[n], recv_sem=tp_recv.at[n],
            device_id={"tp": 1 - tp}, device_id_type=MESH)

    for k, dx in enumerate(QUARTERS):
        g = lax.rem(group + 4 - dx, KV)
        with jax.named_scope(f"agwait{k}"):
            n = (n_lines if dx else n_lines - 1) * AG_ROWS
            pltpu.make_async_copy(full.at[pl.ds(0, n)], full.at[pl.ds(0, n)], ag_recv.at[g]).wait()
            wo_copy(k).wait()
        with jax.named_scope(f"wout{k}"):
            left = jnp.concatenate(
                [jnp.concatenate(
                    [full[pl.ds(g * n_lines * 16 + t * 6 + hd, n_lines, stride=16), :] for t in range(2)], axis=0)
                 for hd in range(6)], axis=1).astype(BF16)
            for n in range(OWNERS):
                res = jnp.dot(left, wo_buf[g, :, n * own:(n + 1) * own], preferred_element_type=F32)
                prods[g, n] = res
                if k == KV - 1:
                    prods[0, n] = (prods[0, n] + prods[1, n]) + (prods[2, n] + prods[3, n])
                    swap(n).start()
    with jax.named_scope("finish"):
        for n in range(OWNERS):
            swap(n).wait()
            at = slice(n * own, (n + 1) * own)
            out_ref[:, at] = (h_ref[:, at].astype(F32) + (prods[0, n] + other[n])).astype(BF16)
    with jax.named_scope("drain"):
        @pl.when(jnp.logical_and(is_kv, jnp.logical_not(is_last)))
        def _():
            wait_for(2, late_recv)
            wait_for(4, early_send)
            wait_for(11, late_send)

        @pl.when(is_last)
        def _():
            wait_for(3, late_recv)
            wait_for(3, early_send)
            wait_for(12, late_send)

        @pl.when(jnp.logical_not(is_kv))
        def _():
            wait_for(3, late_recv)
            wait_for(PLANE - 1, q_send)

        for g in range(KV):
            for i in range(heads_per):
                at = (i * KV + g) * n_seq
                new_ref[at:at + n_seq, :] = recv[g * 4 + 3, :, :, i * 128:(i + 1) * 128].reshape(n_seq, 128)
        pltpu.make_async_copy(rs_others, rs_others, rs_send).wait()
        f_others = full.at[pl.ds(0, (n_sp - 1) * AG_ROWS)]
        pltpu.make_async_copy(f_others, f_others, ag_send).wait()


def cache_kernel(pos_ref, new_ref, k_ref, v_ref, h_ref, k_out, v_out, h_out, k_fix, v_fix, sem):
    n_seq, seq_local = k_ref.shape[:2]
    sp = lax.axis_index("sp")
    base = sp * seq_local
    z_at = sp // PLANE
    trio = ((k_ref, k_fix, k_out), (v_ref, v_fix, v_out))
    hidden = pltpu.make_async_copy(h_ref, h_out, sem.at[2])
    hidden.start()
    for b in range(n_seq):
        at = pos_ref[b] - base
        here = jnp.logical_and(at >= 0, at < seq_local)

        @pl.when(jnp.logical_not(here))
        def _():
            for i, (src, _, dst) in enumerate(trio):
                pltpu.make_async_copy(src.at[b], dst.at[b], sem.at[i]).start()

        @pl.when(here)
        def _():
            for i, (src, fix, dst) in enumerate(trio):
                dz = lax.rem(b % 16 // 4 + 4 - z_at, 4)
                turn = jnp.where(dz == 2, 0, jnp.where(dz == 1, 1, jnp.where(dz == 3, 2, 3)))
                row = i * KV * n_seq + turn * 8 + b // 16 * 4 + b % 4
                fix[b] = src[b]
                fix[b, at] = new_ref[pl.ds(row, KV, stride=n_seq), :].astype(BF16)
                pltpu.make_async_copy(fix.at[b], dst.at[b], sem.at[i]).start()

    for i, (src, _, dst) in enumerate(trio):
        pltpu.make_async_copy(src, dst, sem.at[i]).wait()
    hidden.wait()


def solution(mesh):
    cache_spec = P('dp', 'sp', 'tp', None)
    n_sp = mesh.shape["sp"]

    def local_step(hidden, norm_scale, w_qkv, w_out, k_cache, v_cache, positions):
        n_seq, seq_local, kv, head_dim = k_cache.shape
        d_model = hidden.shape[1]
        width = w_qkv.shape[1] // PLANE
        depth = w_out.shape[0] // kv
        vmem = pl.BlockSpec(memory_space=VMEM)
        smem = pl.BlockSpec(memory_space=pltpu.SMEM)
        hbm = pl.BlockSpec(memory_space=pltpu.HBM)
        half = head_dim // 2
        freq = np.exp(np.arange(half, dtype=np.float32) * np.float32(-2.0 * math.log(500000.0) / head_dim))
        freq = jnp.asarray(np.concatenate([freq, freq])[None].astype(np.float32))
        flat = (n_seq, seq_local * kv, head_dim)
        dma = pltpu.SemaphoreType.DMA

        h_new, new_rows = pl.pallas_call(
            step_kernel,
            out_shape=[jax.ShapeDtypeStruct((n_seq, d_model), BF16), jax.ShapeDtypeStruct((2 * kv * n_seq, head_dim), F32)],
            in_specs=[hbm] * 8,
            out_specs=[vmem, vmem],
            scratch_shapes=[
                pltpu.SMEM((n_seq,), jnp.int32),
                VMEM((n_seq, d_model), BF16),
                VMEM((d_model,), BF16),
                VMEM((1, head_dim), F32),
                dma((4,)),
                VMEM((d_model, width), BF16),
                VMEM((kv, depth, d_model), BF16),
                VMEM(flat, BF16),
                VMEM(flat, BF16),
                VMEM((PLANE, 4, 8, width), F32),
                VMEM((n_seq * 32, head_dim), F32),
                VMEM((n_seq * 32, head_dim), BF16),
                VMEM((n_sp * 16, head_dim), F32),
                VMEM((n_sp * 16, head_dim), F32),
                VMEM((n_sp * 16, head_dim), F32),
                VMEM((kv, OWNERS, n_seq, d_model // OWNERS), F32),
                VMEM((OWNERS, n_seq, d_model // OWNERS), F32),
                dma((K_CHUNKS,)), dma((kv,)), dma((2,)), dma, dma((2,)),
            ] + [dma] * 7 + [dma((kv,)), dma((OWNERS,)), dma((OWNERS,)), pltpu.SemaphoreType.REGULAR],
            compiler_params=pltpu.CompilerParams(
                collective_id=0, has_side_effects=True, vmem_limit_bytes=52 * 1024 * 1024),
            cost_estimate=pl.CostEstimate(flops=60_000_000_000, bytes_accessed=20_000_000, transcendentals=0),
            name="step",
        )(*[pltpu.with_memory_space_constraint(a, pltpu.HBM) for a in (
            positions, hidden, norm_scale, freq, w_qkv, w_out, k_cache.reshape(flat), v_cache.reshape(flat))])

        k_new, v_new, h_out = pl.pallas_call(
            cache_kernel,
            out_shape=[jax.ShapeDtypeStruct(k_cache.shape, BF16)] * 2 + [jax.ShapeDtypeStruct((n_seq, d_model), BF16)],
            in_specs=[smem, vmem, vmem, vmem, vmem],
            out_specs=[hbm, hbm, hbm],
            scratch_shapes=[VMEM(k_cache.shape, BF16)] * 2 + [dma((3,))],
            compiler_params=pltpu.CompilerParams(vmem_limit_bytes=12 * 1024 * 1024),
            name="cache",
        )(positions, new_rows, pltpu.with_memory_space_constraint(k_cache, VMEM),
          pltpu.with_memory_space_constraint(v_cache, VMEM), h_new)
        return h_out, k_new, v_new

    return jax.shard_map(
        local_step,
        mesh=mesh,
        in_specs=(P('dp', None), P(None), P(None, 'tp'), P('tp', None), cache_spec, cache_spec, P('dp')),
        out_specs=(P('dp', None), cache_spec, cache_spec),
        check_vma=False,
    )
```

```python
import itertools
import math

import jax
import jax.numpy as jnp
import numpy as np
from jax import lax
from jax.experimental import pallas as pl
from jax.experimental.pallas import tpu as pltpu
from jax.sharding import PartitionSpec as P

MESH = pl.DeviceIdType.MESH
VMEM = pltpu.VMEM
F32 = jnp.float32
BF16 = jnp.bfloat16
NEG = -3.0e38
PLANE = 16
K_CHUNKS = 6
KV = 4
OWNERS = 8
TURNS = (2, 1, 3, 0)
QUARTERS = (0, 1, 3, 2)
RS_ROWS = 14
AG_ROWS = 12


def farthest_first(dims):
    near = lambda o: sum(min(v, 4 - v) for v in o)
    return sorted((o for o in itertools.product(range(4), repeat=dims) if any(o)), key=lambda o: -near(o))


PLANE_ORDER = farthest_first(2)
CUBE_ORDER = farthest_first(3)


def step_kernel(pos_hbm, h_hbm, scale_hbm, freq_hbm, wq_ref, wo_ref, k_ref, v_ref, out_ref, k_buf, v_buf,
                pos_ref, h_ref, scale_ref, freq_ref, in_sem,
                wq_buf, wk_buf, wl_buf, wo_buf, recv, kvs, xs, xb, part, parts, lhs, mine, shares, full, other,
                wq_sem, wk_sem, wl_sem, wo_sem, kv_sem, q_send, q_recv, early_send, early_recv, late_send, late_recv,
                rs_send, rs_recv, x_send, x_recv, ag_send, ag_recv, tp_send, tp_recv, ready):
    sp = lax.axis_index("sp")
    tp = lax.axis_index("tp")
    n_sp = 64
    line, group = lax.div(sp, KV), lax.rem(sp, KV)
    n_lines = n_sp // KV
    j = lax.rem(sp, PLANE)
    base = sp - j
    y_at, x_at = lax.div(j, 4), lax.rem(j, 4)
    z_at = lax.div(sp, PLANE)
    is_kv = x_at == 3
    n_seq, d_model = h_ref.shape
    width = wk_buf.shape[1]
    rows = d_model // K_CHUNKS
    n_rows = k_ref.shape[1]
    seq_local = n_rows // KV
    depth = wo_buf.shape[0]
    own = d_model // OWNERS
    n_cb = own // 128

    def turn_of(dz):
        return jnp.where(dz == 2, 0, jnp.where(dz == 1, 1, jnp.where(dz == 3, 2, 3)))

    wq_at = pl.multiple_of(y_at * 1024 + 256 + x_at * 128, 128)

    def wq_copy(c):
        return pltpu.make_async_copy(
            wq_ref.at[pl.ds(c * rows, rows), pl.ds(wq_at, 128)], wq_buf.at[pl.ds(c * rows, rows)], wq_sem.at[c])

    wk_copy = pltpu.make_async_copy(
        wq_ref.at[:, pl.ds(pl.multiple_of(y_at * 1024 + 768, 256), width)], wk_buf, wk_sem)

    def wl_copy(g):
        return pltpu.make_async_copy(
            wq_ref.at[:, pl.ds(g * 1024, 256)], wl_buf.at[g // 2, :, pl.ds(g % 2 * 256, 256)], wl_sem.at[g])

    def wo_copy(k):
        return pltpu.make_async_copy(
            wo_ref.at[pl.ds(pl.multiple_of(group * depth, depth) + k * (depth // KV), depth // KV)],
            wo_buf.at[pl.ds(k * (depth // KV), depth // KV)], wo_sem.at[k])

    k_copy = pltpu.make_async_copy(k_ref, k_buf, kv_sem.at[0])
    v_copy = pltpu.make_async_copy(v_ref, v_buf, kv_sem.at[1])
    small = [pltpu.make_async_copy(src, dst, in_sem.at[i]) for i, (src, dst) in enumerate(
        [(h_hbm, h_ref), (pos_hbm, pos_ref), (freq_hbm, freq_ref), (scale_hbm, scale_ref)])]
    for c in small:
        c.start()
    barrier = pltpu.get_barrier_semaphore()

    with jax.named_scope("greet"):
        for dy, dx in PLANE_ORDER:
            peer = base + lax.rem(y_at + dy, 4) * 4 + lax.rem(x_at + dx, 4)
            pl.semaphore_signal(barrier, inc=1, device_id={"sp": peer}, device_id_type=MESH)
        for dz in range(1, 4):
            pl.semaphore_signal(barrier, inc=1, device_id={"sp": lax.rem(sp + dz * PLANE, n_sp)}, device_id_type=MESH)
        pl.semaphore_signal(barrier, inc=1, device_id={"tp": 1 - tp}, device_id_type=MESH)
        for c in range(K_CHUNKS):
            wq_copy(c).start()
        pl.when(is_kv)(wk_copy.start)

    with jax.named_scope("hwait"):
        small[0].wait()
    with jax.named_scope("norm"):
        hidden = h_ref[...].astype(F32)
        centered = hidden - jnp.mean(hidden, axis=-1, keepdims=True)
        var = jnp.mean(centered * centered, axis=-1, keepdims=True)
    with jax.named_scope("inwait"):
        for c in small[1:]:
            c.wait()
        for g in range(KV):
            wl_copy(g).start()
    with jax.named_scope("norm2"):
        u = (centered * lax.rsqrt(var + 1e-5) * scale_ref[...].astype(F32)[None, :]).astype(BF16)
        seq_row = lax.broadcasted_iota(jnp.int32, (n_seq, 128), 0)
        pos = jnp.zeros((n_seq, 128), jnp.int32)
        for b in range(n_seq):
            pos = jnp.where(seq_row == b, pos_ref[b], pos)
        angles = pos.astype(F32) * freq_ref[...]
        cos = jnp.cos(angles)
        sin = jnp.sin(angles)
        sin = jnp.where(lax.broadcasted_iota(jnp.int32, (n_seq, 128), 1) < 64, -sin, sin)

    def clipped(product):
        return jnp.clip(product.astype(BF16), -8.0, 8.0).astype(F32)

    def rotate(piece):
        return (piece * cos + pltpu.roll(piece, 64, 1) * sin).astype(BF16).astype(F32)

    def tile_of(y, z):
        return jnp.concatenate([y[z * 4:z * 4 + 4], y[16 + z * 4:16 + z * 4 + 4]], axis=0)

    with jax.named_scope("qkv"):
        accs = [jnp.zeros((n_seq, 128), F32)] * 2
        for c in range(K_CHUNKS):
            wq_copy(c).wait()
            accs[c % 2] += jnp.dot(u[:, c * rows:(c + 1) * rows], wq_buf[c * rows:(c + 1) * rows, :],
                                   preferred_element_type=F32)
        y = rotate(clipped(accs[0] + accs[1]))
        for z in range(4):
            recv[j, turn_of(lax.rem(z + 4 - z_at, 4))] = tile_of(y, z)
    with jax.named_scope("barrier"):
        pl.semaphore_wait(barrier, PLANE - 1 + 3 + 1)

    def to_plane(dy, dx, block, send_sem, recv_sem):
        peer = base + lax.rem(y_at + dy, 4) * 4 + lax.rem(x_at + dx, 4)
        return pltpu.make_async_remote_copy(
            src_ref=block, dst_ref=block, send_sem=send_sem, recv_sem=recv_sem,
            device_id={"sp": peer}, device_id_type=MESH)

    def wait_for(n, sem):
        pltpu.make_async_copy(kvs.at[pl.ds(0, n)], kvs.at[pl.ds(0, n)], sem).wait()

    def wait_for_halves(n, sem):
        flat_half = xs.at[pl.ds(0, n * n_seq // 2)]
        pltpu.make_async_copy(flat_half, flat_half, sem).wait()

    is_last = jnp.logical_and(is_kv, y_at == 3)
    with jax.named_scope("qsend"):
        for half in range(2):
            for dy, dx in PLANE_ORDER:
                to_plane(dy, dx, recv.at[j, pl.ds(half * 2, 2)], q_send, q_recv.at[half]).start()
        for dz in range(1, 4):
            pl.semaphore_signal(ready, inc=1, device_id={"sp": lax.rem(sp + dz * PLANE, n_sp)}, device_id_type=MESH)
        for g in range(KV):
            for r in (6, 7):
                xs[pl.ds(g * 8 + r, n_seq, stride=32), :] = jnp.zeros((n_seq, 128), F32)

    with jax.named_scope("newkv"):
        @pl.when(is_kv)
        def _():
            wk_copy.wait()
            y = clipped(jnp.dot(u, wk_buf[...], preferred_element_type=F32))
            y = jnp.concatenate([rotate(y[:, :128]), y[:, 128:]], axis=1)
            for z in range(4):
                kvs[y_at, turn_of(lax.rem(z + 4 - z_at, 4))] = tile_of(y, z)
            for dy in (2, 1, 3, 0):
                @pl.when(jnp.logical_or(dy != 0, y_at != 3))
                def _():
                    to_plane(dy, lax.rem(y_at + 1, 4), kvs.at[y_at], early_send, early_recv).start()

    with jax.named_scope("local"):
        for pair in range(2):
            wl_copy(pair * 2).wait()
            wl_copy(pair * 2 + 1).wait()
            if pair == 0:
                k_copy.start()
                v_copy.start()
            y = clipped(jnp.dot(u, wl_buf[pair], preferred_element_type=F32))
            for i in range(4):
                piece = rotate(y[:, i * 128:(i + 1) * 128])
                for z in range(4):
                    at = turn_of(lax.rem(z + 4 - z_at, 4)) * 256 + (pair * 2 + i // 2) * 8 + i % 2
                    xs[pl.ds(at, 8, stride=32), :] = tile_of(piece, z)
        for k in range(KV):
            wo_copy(k).start()

    def half_queries(half):
        with jax.named_scope(f"qwait{half}"):
            wait_for_halves(PLANE - 1, q_recv.at[half])
        with jax.named_scope("spread"):
            for turn in (half * 2, half * 2 + 1):
                for blk in range(PLANE):
                    xs[pl.ds(turn * 256 + blk // 4 * 8 + 2 + blk % 4, 8, stride=32), :] = recv[blk, turn]
                xb[turn * 256:(turn + 1) * 256, :] = xs[turn * 256:(turn + 1) * 256, :].astype(BF16)

    row8 = lax.broadcasted_iota(jnp.int32, (32, 128), 0) % 8
    lane32 = lax.broadcasted_iota(jnp.int32, (32, 128), 1)

    def as_rows(cols, n):
        tiles = sum(jnp.where((lane32 == row8 + 8 * t)[:8 * n], c, 0.0) for t, c in enumerate(cols)).reshape(n, 8, 128)
        return jnp.broadcast_to(jnp.sum(tiles, axis=1, keepdims=True), (n, 8, 128)).reshape(8 * n, 128)

    with jax.named_scope("kvwait"):
        k_copy.wait()
        v_copy.wait()
    row = lax.broadcasted_iota(jnp.int32, (32, n_rows), 0)
    col = lax.broadcasted_iota(jnp.int32, (32, n_rows), 1)
    seq_of = jnp.where(col % KV == row // 8, col // KV + sp * seq_local, 1 << 30)
    scale = 128 ** -0.5

    def line_at(turn, i):
        return lax.rem(z_at + TURNS[turn], 4) * 4 + lax.rem(y_at + TURNS[i], 4)

    def scores(turn):
        out = []
        for i in range(4):
            for t in range(2):
                at = (turn * 8 + t * 4 + lax.rem(y_at + TURNS[i], 4)) * 32
                b = line_at(turn, i) + 16 * t
                q = xb[pl.ds(pl.multiple_of(at, 32), 32), :]
                s = lax.dot_general(q, k_buf[b], (((1,), (1,)), ((), ())), preferred_element_type=F32) * scale
                out.append(jnp.where(seq_of < pos_ref[b], s, NEG))
        return out

    def values(turn, held):
        for i in range(4):
            ln = line_at(turn, i)
            stats, outs = [], []
            for t in range(2):
                s = held[i * 2 + t]
                m = jnp.max(s, axis=1, keepdims=True)
                e = jnp.exp(s - m)
                stats.append((m, jnp.sum(e, axis=1, keepdims=True)))
                outs.append(jnp.dot(e.astype(BF16), v_buf[ln + 16 * t], preferred_element_type=F32))
            (m0, l0), (m1, l1) = stats
            first = jnp.where(row8 == 6, as_rows((m0, m1), KV), jnp.where(row8 == 7, as_rows((l0, l1), KV), outs[0]))
            for g in range(KV):
                at = pl.multiple_of((ln * KV + g) * 16, 16)
                part[pl.ds(at, 8), :] = first[g * 8:(g + 1) * 8]
                part[pl.ds(at + 8, 8), :] = outs[1][g * 8:(g + 1) * 8]

    def send_partials(turn):
        for i in range(4):
            ln = line_at(turn, i)
            for d in TURNS:
                if turn == 3 and i == 3 and d == 0:
                    continue
                to = lax.rem(group + d, KV)
                pltpu.make_async_remote_copy(
                    src_ref=part.at[pl.ds(pl.multiple_of((ln * KV + to) * 16, 16), RS_ROWS)],
                    dst_ref=parts.at[pl.ds(pl.multiple_of(sp * 16, 16), RS_ROWS)], send_sem=rs_send,
                    recv_sem=rs_recv, device_id={"sp": ln * KV + to}, device_id_type=MESH).start()

    half_queries(0)
    with jax.named_scope("ready"):
        pl.semaphore_wait(ready, 3)
    with jax.named_scope("attn0"):
        held = scores(0)
        ahead = scores(1)
        values(0, held)
        send_partials(0)
        values(1, ahead)
        send_partials(1)
    half_queries(1)
    with jax.named_scope("attn1"):
        held = scores(2)
        ahead = scores(3)
        values(2, held)
        send_partials(2)
        values(3, ahead)
        send_partials(3)
        parts[pl.ds(pl.multiple_of(sp * 16, 16), 16), :] = part[pl.ds(pl.multiple_of(sp * 16, 16), 16), :]

    with jax.named_scope("newrow"):
        @pl.when(jnp.logical_not(is_last))
        def _():
            wait_for(1, early_recv)

        for i in range(2):
            xs[pl.ds(3 * 256 + group * 8 + 6 + i, 8, stride=32), :] = kvs[group, 3, :, i * 128:(i + 1) * 128]
        cols, v_new = [], []
        for t in range(2):
            tile = xs[pl.ds(pl.multiple_of((24 + t * 4 + y_at) * 32 + group * 8, 8), 8), :]
            cols.append(jnp.sum(tile * tile[6:7, :], axis=1, keepdims=True) * scale)
            v_new.append(tile[7:8, :])
        m_new = as_rows(cols, 1)[:1]

    rs_others = parts.at[pl.ds(0, (n_sp - 1) * RS_ROWS)]
    with jax.named_scope("rswait"):
        pltpu.make_async_copy(rs_others, rs_others, rs_recv).wait()

    with jax.named_scope("merge"):
        lane = lax.broadcasted_iota(jnp.int32, (1, 128), 1)
        m = parts[pl.ds(6, n_sp, stride=16), :]
        l = parts[pl.ds(7, n_sp, stride=16), :]
        top = jnp.maximum(jnp.max(m, axis=0, keepdims=True), m_new)
        f = jnp.exp(m - top)
        f_new = jnp.exp(m_new - top)
        real = jnp.logical_and(lane < 16, lane % 8 < 6)
        den = jnp.where(real, jnp.sum(f * l, axis=0, keepdims=True) + f_new, 1.0)
        wt = (jnp.concatenate([f, jnp.broadcast_to(f_new, (8, 128))], axis=0) / den).T
        lhs[...] = jnp.zeros_like(lhs)
        for t in range(2):
            w8 = wt[t * 8:(t + 1) * 8]
            sums = [w8[:, n_sp:n_sp + 1] * v_new[t]] + [jnp.zeros((8, 128), F32)] * 3
            for s in range(n_sp):
                sums[s % 4] += w8[:, s:s + 1] * parts[s * 16 + t * 8:s * 16 + t * 8 + 8, :]
            acc = (sums[0] + sums[1]) + (sums[2] + sums[3])
            for hd in range(6):
                lhs[t:t + 1, hd * 128:(hd + 1) * 128] = acc[hd:hd + 1, :]

    me = group * 2 + tp
    with jax.named_scope("wout"):
        for k in range(KV):
            wo_copy(k).wait()
        left = lhs[...].astype(BF16)

        order = [(dg, dt) for dg in TURNS for dt in (1, 0)]

        def product(k):
            owner = lax.rem(group + order[k][0], KV) * 2 + (1 - tp if order[k][1] else tp)
            at = pl.multiple_of(owner * own, own)
            return owner, jnp.dot(left, wo_buf[:, pl.ds(at, own)], preferred_element_type=F32)

        held = product(0)
        for k in range(OWNERS):
            ahead = product(k + 1) if k + 1 < OWNERS else None
            owner, res = held
            buf = mine if k < OWNERS - 1 else shares
            at = pl.multiple_of(owner * 16, 16)
            for t in range(2):
                for cb in range(n_cb):
                    buf[pl.ds(at + t * n_cb + cb, 1), :] = res[t:t + 1, cb * 128:(cb + 1) * 128]
            if k < OWNERS - 1:
                pltpu.make_async_remote_copy(
                    src_ref=mine.at[pl.ds(at, AG_ROWS)],
                    dst_ref=shares.at[pl.ds(pl.multiple_of(me * 16, 16), AG_ROWS)], send_sem=x_send, recv_sem=x_recv,
                    device_id={"tp": lax.rem(owner, 2), "sp": line * KV + lax.div(owner, 2)},
                    device_id_type=MESH).start()
            held = ahead

    with jax.named_scope("forward"):
        for dx in (2, 1, 3):
            to = lax.rem(x_at + dx, 4)

            @pl.when(jnp.logical_or(to != 3, y_at != x_at))
            def _():
                pltpu.make_async_remote_copy(
                    src_ref=kvs.at[group], dst_ref=kvs.at[group], send_sem=late_send,
                    recv_sem=late_recv, device_id={"sp": line * 4 + to}, device_id_type=MESH).start()

    x_others = shares.at[pl.ds(0, (OWNERS - 1) * AG_ROWS)]
    quarter_rows = n_lines * 16
    slot = pl.multiple_of((group * n_lines + line) * 16, 16)
    mine_rows = full.at[pl.ds(slot, AG_ROWS)]

    with jax.named_scope("xwait"):
        pltpu.make_async_copy(x_others, x_others, x_recv).wait()
    with jax.named_scope("agsend"):
        total = shares[0:16, :]
        for s in range(1, OWNERS):
            total += shares[s * 16:(s + 1) * 16, :]
        full[pl.ds(slot, 16), :] = total
        zs = [lax.rem(z_at + d, 4) * 16 for d in range(4)]
        ys = [lax.rem(y_at + d, 4) * 4 for d in range(4)]
        xs_ = [lax.rem(x_at + d, 4) for d in range(4)]
        for dz, dy, dx in CUBE_ORDER:
            pltpu.make_async_remote_copy(
                src_ref=mine_rows, dst_ref=mine_rows, send_sem=ag_send, recv_sem=ag_recv.at[group],
                device_id={"sp": zs[dz] + ys[dy] + xs_[dx]}, device_id_type=MESH).start()

    with jax.named_scope("latewait"):
        @pl.when(jnp.logical_and(is_kv, jnp.logical_not(is_last)))
        def _():
            wait_for(2, late_recv)

        @pl.when(jnp.logical_or(jnp.logical_not(is_kv), is_last))
        def _():
            wait_for(3, late_recv)
    with jax.named_scope("update"):
        sub = lax.broadcasted_iota(jnp.int32, (8, 128), 0)

        def update(turn, carry):
            dz = jnp.where(turn == 0, 2, jnp.where(turn == 1, 1, jnp.where(turn == 2, 3, 0)))
            for t in range(2):
                for y in range(4):
                    b = t * 16 + lax.rem(z_at + dz, 4) * 4 + y
                    at = pos_ref[b] - sp * seq_local
                    for i, buf in enumerate((k_buf, v_buf)):
                        new = jnp.zeros((8, 128), F32)
                        for g in range(KV):
                            source = kvs[g, turn, t * 4 + y:t * 4 + y + 1, i * 128:(i + 1) * 128]
                            new = jnp.where(sub % KV == g, source, new)
                        old = buf[b].astype(F32)
                        buf[b] = jnp.concatenate(
                            [jnp.where(sub // KV == at - 2 * v, new, old[v * 8:(v + 1) * 8])
                             for v in range(n_rows // 8)], axis=0).astype(BF16)
            return carry

        lax.fori_loop(0, 4, update, 0)

    def quarter(dx):
        g = lax.rem(group + 4 - dx, KV)
        at = pl.ds(pl.multiple_of(g * quarter_rows, quarter_rows), quarter_rows)
        return g, pltpu.make_async_remote_copy(
            src_ref=full.at[at], dst_ref=other.at[at], send_sem=tp_send.at[g], recv_sem=tp_recv.at[g],
            device_id={"tp": 1 - tp}, device_id_type=MESH)

    def finish(buf, g, core):
        for cb in range(n_cb):
            at = pl.ds(pl.multiple_of((g * 2 + core) * own + cb * 128, 128), 128)
            for t in range(2):
                slab = buf[pl.ds(g * quarter_rows + t * n_cb + cb, n_lines, stride=16), :]
                out_ref[t * 16:(t + 1) * 16, at] = (h_ref[t * 16:(t + 1) * 16, at].astype(F32) + slab).astype(BF16)

    with jax.named_scope("agwait"):
        for dx in QUARTERS:
            g, swap = quarter(dx)
            n = (n_lines if dx else n_lines - 1) * AG_ROWS
            pltpu.make_async_copy(full.at[pl.ds(0, n)], full.at[pl.ds(0, n)], ag_recv.at[g]).wait()
            swap.start()
            finish(full, g, tp)
    with jax.named_scope("swapwait"):
        for dx in QUARTERS:
            g, swap = quarter(dx)
            swap.wait()
            finish(other, g, 1 - tp)

    with jax.named_scope("drain"):
        @pl.when(jnp.logical_and(is_kv, jnp.logical_not(is_last)))
        def _():
            wait_for(4, early_send)

        @pl.when(is_last)
        def _():
            wait_for(3, early_send)

        wait_for_halves(2 * (PLANE - 1), q_send)
        returns = jnp.logical_and(y_at == x_at, jnp.logical_not(is_kv))

        @pl.when(returns)
        def _():
            wait_for(2, late_send)

        @pl.when(jnp.logical_not(returns))
        def _():
            wait_for(3, late_send)

        pltpu.make_async_copy(rs_others, rs_others, rs_send).wait()

        pltpu.make_async_copy(x_others, x_others, x_send).wait()
        f_others = full.at[pl.ds(0, (n_sp - 1) * AG_ROWS)]
        pltpu.make_async_copy(f_others, f_others, ag_send).wait()


def store_kernel(*refs):
    n = len(refs) // 2
    sem = refs[-1]
    copies = [pltpu.make_async_copy(refs[i], refs[n + i], sem.at[i]) for i in range(n)]
    for c in copies:
        c.start()
    for c in copies:
        c.wait()


def solution(mesh):
    cache_spec = P('dp', 'sp', 'tp', None)
    n_sp = mesh.shape["sp"]

    def local_step(hidden, norm_scale, w_qkv, w_out, k_cache, v_cache, positions):
        n_seq, seq_local, kv, head_dim = k_cache.shape
        d_model = hidden.shape[1]
        depth = w_out.shape[0] // kv
        vmem = pl.BlockSpec(memory_space=VMEM)
        hbm = pl.BlockSpec(memory_space=pltpu.HBM)
        half = head_dim // 2
        freq = np.exp(np.arange(half, dtype=np.float32) * np.float32(-2.0 * math.log(500000.0) / head_dim))
        freq = jnp.asarray(np.concatenate([freq, freq])[None].astype(np.float32))
        flat = (n_seq, seq_local * kv, head_dim)
        dma = pltpu.SemaphoreType.DMA

        hidden_type = jax.ShapeDtypeStruct((n_seq, d_model), BF16)
        results = pl.pallas_call(
            step_kernel,
            out_shape=[hidden_type, jax.ShapeDtypeStruct(flat, BF16), jax.ShapeDtypeStruct(flat, BF16)],
            in_specs=[hbm] * 8,
            out_specs=[vmem, vmem, vmem],
            scratch_shapes=[
                pltpu.SMEM((n_seq,), jnp.int32),
                VMEM((n_seq, d_model), BF16),
                VMEM((d_model,), BF16),
                VMEM((1, head_dim), F32),
                dma((4,)),
                VMEM((d_model, head_dim), BF16),
                VMEM((d_model, 2 * head_dim), BF16),
                VMEM((kv // 2, d_model, 4 * head_dim), BF16),
                VMEM((depth, d_model), BF16),
                VMEM((PLANE, 4, 8, head_dim), F32),
                VMEM((kv, 4, 8, 2 * head_dim), F32),
                VMEM((n_seq * 32, head_dim), F32),
                VMEM((n_seq * 32, head_dim), BF16),
                VMEM((n_sp * 16, head_dim), F32),
                VMEM((n_sp * 16, head_dim), F32),
                VMEM((8, depth), F32),
                VMEM((OWNERS * 16, head_dim), F32),
                VMEM((OWNERS * 16, head_dim), F32),
                VMEM((n_sp * 16, head_dim), F32),
                VMEM((n_sp * 16, head_dim), F32),
                dma((K_CHUNKS,)), dma, dma((kv,)), dma((kv,)), dma((2,)), dma, dma((2,)),
            ] + [dma] * 9 + [dma((kv,))] * 3 + [pltpu.SemaphoreType.REGULAR],
            compiler_params=pltpu.CompilerParams(
                collective_id=0, has_side_effects=True, vmem_limit_bytes=48 * 1024 * 1024),
            cost_estimate=pl.CostEstimate(flops=60_000_000_000, bytes_accessed=20_000_000, transcendentals=0),
            name="step",
        )(*[pltpu.with_memory_space_constraint(a, pltpu.HBM) for a in (
            positions, hidden, norm_scale, freq, w_qkv, w_out, k_cache.reshape(flat), v_cache.reshape(flat))])

        h_out, k_new, v_new = pl.pallas_call(
            store_kernel,
            out_shape=[hidden_type, jax.ShapeDtypeStruct(flat, BF16), jax.ShapeDtypeStruct(flat, BF16)],
            in_specs=[vmem] * 3,
            out_specs=[hbm] * 3,
            scratch_shapes=[dma((3,))],
            compiler_params=pltpu.CompilerParams(vmem_limit_bytes=8 * 1024 * 1024),
            name="store",
        )(*[pltpu.with_memory_space_constraint(a, VMEM) for a in results])
        k_new, v_new = k_new.reshape(k_cache.shape), v_new.reshape(v_cache.shape)
        return h_out, k_new, v_new

    return jax.shard_map(
        local_step,
        mesh=mesh,
        in_specs=(P('dp', None), P(None), P(None, 'tp'), P('tp', None), cache_spec, cache_spec, P('dp')),
        out_specs=(P('dp', None), cache_spec, cache_spec),
        check_vma=False,
    )
```

```python
import itertools
import math

import jax
import jax.numpy as jnp
import numpy as np
from jax import lax
from jax.experimental import pallas as pl
from jax.experimental.pallas import tpu as pltpu
from jax.sharding import PartitionSpec as P

MESH = pl.DeviceIdType.MESH
VMEM = pltpu.VMEM
F32 = jnp.float32
BF16 = jnp.bfloat16
NEG = -3.0e38
LEAST = -1.0e38
PLANE = 16
K_CHUNKS = 6
KV = 4
OWNERS = 8
TURNS = (2, 1, 3, 0)
QUARTERS = (0, 1, 3, 2)
RS_ROWS = 13
AG_ROWS = 12


def farthest_first(dims):
    near = lambda o: sum(min(v, 4 - v) for v in o)
    return sorted((o for o in itertools.product(range(4), repeat=dims) if any(o)), key=lambda o: -near(o))


PLANE_ORDER = farthest_first(2)
CUBE_ORDER = farthest_first(3)


def step_kernel(pos_hbm, h_hbm, scale_hbm, freq_hbm, wq_ref, wo_ref, k_ref, v_ref, out_ref, k_buf, v_buf,
                pos_ref, h_ref, scale_ref, freq_ref, in_sem,
                wq_buf, wk_buf, wl_buf, wo_buf, recv, kvs, xs, xb, part, parts, lhs, mine, shares, full, other,
                wq_sem, wk_sem, wl_sem, wo_sem, kv_sem, q_send, q_recv, early_send, early_recv, late_send, late_recv,
                rs_send, rs_recv, x_send, x_recv, ag_send, ag_recv, tp_send, tp_recv, ready):
    sp = lax.axis_index("sp")
    tp = lax.axis_index("tp")
    n_sp = 64
    line, group = lax.div(sp, KV), lax.rem(sp, KV)
    n_lines = n_sp // KV
    j = lax.rem(sp, PLANE)
    base = sp - j
    y_at, x_at = lax.div(j, 4), lax.rem(j, 4)
    z_at = lax.div(sp, PLANE)
    is_kv = x_at == 3
    n_seq, d_model = h_ref.shape
    width = wk_buf.shape[1]
    rows = d_model // K_CHUNKS
    n_rows = k_ref.shape[1]
    seq_local = n_rows // KV
    depth = wo_buf.shape[0]
    own = d_model // OWNERS
    n_cb = own // 128

    def turn_of(dz):
        return jnp.where(dz == 2, 0, jnp.where(dz == 1, 1, jnp.where(dz == 3, 2, 3)))

    wq_at = pl.multiple_of(y_at * 1024 + 256 + x_at * 128, 128)

    def wq_copy(c):
        return pltpu.make_async_copy(
            wq_ref.at[pl.ds(c * rows, rows), pl.ds(wq_at, 128)], wq_buf.at[pl.ds(c * rows, rows)], wq_sem.at[c])

    wk_copy = pltpu.make_async_copy(
        wq_ref.at[:, pl.ds(pl.multiple_of(y_at * 1024 + 768, 256), width)], wk_buf, wk_sem)

    def wl_copy(g):
        return pltpu.make_async_copy(
            wq_ref.at[:, pl.ds(g * 1024, 256)], wl_buf.at[g // 2, :, pl.ds(g % 2 * 256, 256)], wl_sem.at[g])

    def wo_copy(k):
        return pltpu.make_async_copy(
            wo_ref.at[pl.ds(pl.multiple_of(group * depth, depth) + k * (depth // KV), depth // KV)],
            wo_buf.at[pl.ds(k * (depth // KV), depth // KV)], wo_sem.at[k])

    k_copy = pltpu.make_async_copy(k_ref, k_buf, kv_sem.at[0])
    v_copy = pltpu.make_async_copy(v_ref, v_buf, kv_sem.at[1])
    small = [pltpu.make_async_copy(src, dst, in_sem.at[i]) for i, (src, dst) in enumerate(
        [(h_hbm, h_ref), (pos_hbm, pos_ref), (freq_hbm, freq_ref), (scale_hbm, scale_ref)])]
    for c in small:
        c.start()
    barrier = pltpu.get_barrier_semaphore()

    with jax.named_scope("greet"):
        for dy, dx in PLANE_ORDER:
            peer = base + lax.rem(y_at + dy, 4) * 4 + lax.rem(x_at + dx, 4)
            pl.semaphore_signal(barrier, inc=1, device_id={"sp": peer}, device_id_type=MESH)
        for dz in range(1, 4):
            pl.semaphore_signal(barrier, inc=1, device_id={"sp": lax.rem(sp + dz * PLANE, n_sp)}, device_id_type=MESH)
        pl.semaphore_signal(barrier, inc=1, device_id={"tp": 1 - tp}, device_id_type=MESH)
        for c in range(K_CHUNKS):
            wq_copy(c).start()
        pl.when(is_kv)(wk_copy.start)

    with jax.named_scope("hwait"):
        small[0].wait()
        for g in range(KV):
            wl_copy(g).start()
    with jax.named_scope("norm"):
        hidden = h_ref[...].astype(F32)
        centered = hidden - jnp.mean(hidden, axis=-1, keepdims=True)
        var = jnp.mean(centered * centered, axis=-1, keepdims=True)
    with jax.named_scope("inwait"):
        for c in small[1:]:
            c.wait()
    with jax.named_scope("norm2"):
        u = (centered * lax.rsqrt(var + 1e-5) * scale_ref[...].astype(F32)[None, :]).astype(BF16)
        seq_row = lax.broadcasted_iota(jnp.int32, (n_seq, 128), 0)
        pos = jnp.zeros((n_seq, 128), jnp.int32)
        for b in range(n_seq):
            pos = jnp.where(seq_row == b, pos_ref[b], pos)
        angles = pos.astype(F32) * freq_ref[...]
        cos = jnp.cos(angles)
        sin = jnp.sin(angles)
        sin = jnp.where(lax.broadcasted_iota(jnp.int32, (n_seq, 128), 1) < 64, -sin, sin)

    def clipped(product):
        return jnp.clip(product.astype(BF16), -8.0, 8.0).astype(F32)

    def rotate(piece):
        return (piece * cos + pltpu.roll(piece, 64, 1) * sin).astype(BF16).astype(F32)

    def tile_of(y, z):
        return jnp.concatenate([y[z * 4:z * 4 + 4], y[16 + z * 4:16 + z * 4 + 4]], axis=0)

    with jax.named_scope("qkv"):
        accs = [jnp.zeros((n_seq, 128), F32)] * 2
        for c in range(K_CHUNKS):
            wq_copy(c).wait()
            accs[c % 2] += jnp.dot(u[:, c * rows:(c + 1) * rows], wq_buf[c * rows:(c + 1) * rows, :],
                                   preferred_element_type=F32)
        y = rotate(clipped(accs[0] + accs[1]))
        for z in range(4):
            recv[j, turn_of(lax.rem(z + 4 - z_at, 4))] = tile_of(y, z)
    with jax.named_scope("barrier"):
        pl.semaphore_wait(barrier, PLANE - 1 + 3 + 1)

    def to_plane(dy, dx, block, send_sem, recv_sem):
        peer = base + lax.rem(y_at + dy, 4) * 4 + lax.rem(x_at + dx, 4)
        return pltpu.make_async_remote_copy(
            src_ref=block, dst_ref=block, send_sem=send_sem, recv_sem=recv_sem,
            device_id={"sp": peer}, device_id_type=MESH)

    def wait_for(n, sem):
        pltpu.make_async_copy(kvs.at[pl.ds(0, n)], kvs.at[pl.ds(0, n)], sem).wait()

    def wait_for_halves(n, sem):
        flat_half = xs.at[pl.ds(0, n * n_seq // 2)]
        pltpu.make_async_copy(flat_half, flat_half, sem).wait()

    is_last = jnp.logical_and(is_kv, y_at == 3)
    with jax.named_scope("qsend"):
        for half in range(2):
            for dy, dx in PLANE_ORDER:
                to_plane(dy, dx, recv.at[j, pl.ds(half * 2, 2)], q_send, q_recv.at[half]).start()
        for dz in range(1, 4):
            pl.semaphore_signal(ready, inc=1, device_id={"sp": lax.rem(sp + dz * PLANE, n_sp)}, device_id_type=MESH)
        for g in range(KV):
            for r in (6, 7):
                xs[pl.ds(g * 8 + r, n_seq, stride=32), :] = jnp.zeros((n_seq, 128), F32)

    with jax.named_scope("newkv"):
        @pl.when(is_kv)
        def _():
            wk_copy.wait()
            y = clipped(jnp.dot(u, wk_buf[...], preferred_element_type=F32))
            y = jnp.concatenate([rotate(y[:, :128]), y[:, 128:]], axis=1)
            for z in range(4):
                kvs[y_at, turn_of(lax.rem(z + 4 - z_at, 4))] = tile_of(y, z)
            for dy in (2, 1, 3, 0):
                @pl.when(jnp.logical_or(dy != 0, y_at != 3))
                def _():
                    to_plane(dy, lax.rem(y_at + 1, 4), kvs.at[y_at], early_send, early_recv).start()

    with jax.named_scope("local"):
        for pair in range(2):
            wl_copy(pair * 2).wait()
            wl_copy(pair * 2 + 1).wait()
            if pair == 0:
                k_copy.start()
                v_copy.start()
            y = clipped(jnp.dot(u, wl_buf[pair], preferred_element_type=F32))
            for i in range(4):
                piece = rotate(y[:, i * 128:(i + 1) * 128])
                for z in range(4):
                    at = turn_of(lax.rem(z + 4 - z_at, 4)) * 256 + (pair * 2 + i // 2) * 8 + i % 2
                    xs[pl.ds(at, 8, stride=32), :] = tile_of(piece, z)
        for k in range(KV):
            wo_copy(k).start()

    def half_queries(half):
        with jax.named_scope(f"qwait{half}"):
            wait_for_halves(PLANE - 1, q_recv.at[half])
        with jax.named_scope("spread"):
            for turn in (half * 2, half * 2 + 1):
                for blk in range(PLANE):
                    xs[pl.ds(turn * 256 + blk // 4 * 8 + 2 + blk % 4, 8, stride=32), :] = recv[blk, turn]
                xb[turn * 256:(turn + 1) * 256, :] = xs[turn * 256:(turn + 1) * 256, :].astype(BF16)

    row8 = lax.broadcasted_iota(jnp.int32, (32, 128), 0) % 8
    lane32 = lax.broadcasted_iota(jnp.int32, (32, 128), 1)

    def as_rows(cols, n):
        tiles = sum(jnp.where((lane32 == row8 + 8 * t)[:8 * n], c, 0.0) for t, c in enumerate(cols)).reshape(n, 8, 128)
        return jnp.broadcast_to(jnp.sum(tiles, axis=1, keepdims=True), (n, 8, 128)).reshape(8 * n, 128)

    with jax.named_scope("kvwait"):
        k_copy.wait()
        v_copy.wait()
    row = lax.broadcasted_iota(jnp.int32, (32, n_rows), 0)
    col = lax.broadcasted_iota(jnp.int32, (32, n_rows), 1)
    seq_of = jnp.where(col % KV == row // 8, col // KV + sp * seq_local, 1 << 30)
    scale = 128 ** -0.5

    def line_at(turn, i):
        return lax.rem(z_at + TURNS[turn], 4) * 4 + lax.rem(y_at + TURNS[i], 4)

    def scores(turn):
        out = []
        for i in range(4):
            for t in range(2):
                at = (turn * 8 + t * 4 + lax.rem(y_at + TURNS[i], 4)) * 32
                b = line_at(turn, i) + 16 * t
                q = xb[pl.ds(pl.multiple_of(at, 32), 32), :]
                s = lax.dot_general(q, k_buf[b], (((1,), (1,)), ((), ())), preferred_element_type=F32) * scale
                out.append(jnp.where(seq_of < pos_ref[b], s, NEG))
        return out

    def values(turn, held):
        for i in range(4):
            ln = line_at(turn, i)
            stats, outs = [], []
            for t in range(2):
                s = held[i * 2 + t]
                m = jnp.maximum(jnp.max(s, axis=1, keepdims=True), LEAST)
                e = jnp.exp(s - m)
                stats.append((m, jnp.sum(e, axis=1, keepdims=True)))
                outs.append(jnp.dot(e.astype(BF16), v_buf[ln + 16 * t], preferred_element_type=F32))
            (m0, l0), (m1, l1) = stats
            first = jnp.where(row8 == 6, as_rows((m0, m1, l0, l1), KV), outs[0])
            for g in range(KV):
                at = pl.multiple_of((ln * KV + g) * 16, 16)
                part[pl.ds(at, 8), :] = first[g * 8:(g + 1) * 8]
                part[pl.ds(at + 7, 6), :] = outs[1][g * 8:g * 8 + 6]

    def send_partials(turn):
        for i in range(4):
            ln = line_at(turn, i)
            for d in TURNS:
                if turn == 3 and i == 3 and d == 0:
                    continue
                to = lax.rem(group + d, KV)
                pltpu.make_async_remote_copy(
                    src_ref=part.at[pl.ds(pl.multiple_of((ln * KV + to) * 16, 16), RS_ROWS)],
                    dst_ref=parts.at[pl.ds(pl.multiple_of(sp * 16, 16), RS_ROWS)], send_sem=rs_send,
                    recv_sem=rs_recv, device_id={"sp": ln * KV + to}, device_id_type=MESH).start()

    half_queries(0)
    with jax.named_scope("ready"):
        pl.semaphore_wait(ready, 3)
    with jax.named_scope("attn0"):
        held = scores(0)
        ahead = scores(1)
        values(0, held)
        send_partials(0)
        values(1, ahead)
        send_partials(1)
    half_queries(1)
    with jax.named_scope("attn1"):
        held = scores(2)
        ahead = scores(3)
        values(2, held)
        send_partials(2)
        values(3, ahead)
        send_partials(3)
        parts[pl.ds(pl.multiple_of(sp * 16, 16), 16), :] = part[pl.ds(pl.multiple_of(sp * 16, 16), 16), :]

    with jax.named_scope("newrow"):
        @pl.when(jnp.logical_not(is_last))
        def _():
            wait_for(1, early_recv)

        for i in range(2):
            xs[pl.ds(3 * 256 + group * 8 + 6 + i, 8, stride=32), :] = kvs[group, 3, :, i * 128:(i + 1) * 128]
        cols, v_new = [], []
        for t in range(2):
            tile = xs[pl.ds(pl.multiple_of((24 + t * 4 + y_at) * 32 + group * 8, 8), 8), :]
            cols.append(jnp.sum(tile * tile[6:7, :], axis=1, keepdims=True) * scale)
            v_new.append(tile[7:8, :])
        m_new = as_rows(cols, 1)[:1]

    rs_others = parts.at[pl.ds(0, (n_sp - 1) * RS_ROWS)]
    with jax.named_scope("rswait"):
        pltpu.make_async_copy(rs_others, rs_others, rs_recv).wait()

    with jax.named_scope("merge"):
        lane = lax.broadcasted_iota(jnp.int32, (1, 128), 1)
        m = parts[pl.ds(6, n_sp, stride=16), :]
        l = pltpu.roll(m, 112, 1)
        top = jnp.maximum(jnp.max(m, axis=0, keepdims=True), m_new)
        f = jnp.exp(m - top)
        f_new = jnp.exp(m_new - top)
        real = jnp.logical_and(lane < 16, lane % 8 < 6)
        den = jnp.where(real, jnp.sum(f * l, axis=0, keepdims=True) + f_new, 1.0)
        wt = (jnp.concatenate([f, jnp.broadcast_to(f_new, (8, 128))], axis=0) / den).T
        lhs[...] = jnp.zeros_like(lhs)
        for t in range(2):
            w8 = wt[t * 8:(t + 1) * 8]
            sums = [w8[:, n_sp:n_sp + 1] * v_new[t]] + [jnp.zeros((8, 128), F32)] * 3
            for s in range(n_sp):
                sums[s % 4] += w8[:, s:s + 1] * parts[s * 16 + t * 7:s * 16 + t * 7 + 8, :]
            acc = (sums[0] + sums[1]) + (sums[2] + sums[3])
            for hd in range(6):
                lhs[t:t + 1, hd * 128:(hd + 1) * 128] = acc[hd:hd + 1, :]

    me = group * 2 + tp
    with jax.named_scope("wout"):
        for k in range(KV):
            wo_copy(k).wait()
        left = lhs[...].astype(BF16)

        order = [(dg, dt) for dg in TURNS for dt in (1, 0)]

        def product(k):
            owner = lax.rem(group + order[k][0], KV) * 2 + (1 - tp if order[k][1] else tp)
            at = pl.multiple_of(owner * own, own)
            return owner, jnp.dot(left, wo_buf[:, pl.ds(at, own)], preferred_element_type=F32)

        held = product(0)
        for k in range(OWNERS):
            ahead = product(k + 1) if k + 1 < OWNERS else None
            owner, res = held
            buf = mine if k < OWNERS - 1 else shares
            at = pl.multiple_of(owner * 16, 16)
            for t in range(2):
                for cb in range(n_cb):
                    buf[pl.ds(at + t * n_cb + cb, 1), :] = res[t:t + 1, cb * 128:(cb + 1) * 128]
            if k < OWNERS - 1:
                pltpu.make_async_remote_copy(
                    src_ref=mine.at[pl.ds(at, AG_ROWS)],
                    dst_ref=shares.at[pl.ds(pl.multiple_of(me * 16, 16), AG_ROWS)], send_sem=x_send, recv_sem=x_recv,
                    device_id={"tp": lax.rem(owner, 2), "sp": line * KV + lax.div(owner, 2)},
                    device_id_type=MESH).start()
            held = ahead

    with jax.named_scope("forward"):
        for dx in (2, 1, 3):
            to = lax.rem(x_at + dx, 4)

            @pl.when(jnp.logical_or(to != 3, y_at != x_at))
            def _():
                pltpu.make_async_remote_copy(
                    src_ref=kvs.at[group], dst_ref=kvs.at[group], send_sem=late_send,
                    recv_sem=late_recv, device_id={"sp": line * 4 + to}, device_id_type=MESH).start()

    x_others = shares.at[pl.ds(0, (OWNERS - 1) * AG_ROWS)]
    quarter_rows = n_lines * 16
    slot = pl.multiple_of((group * n_lines + line) * 16, 16)
    mine_rows = full.at[pl.ds(slot, AG_ROWS)]

    with jax.named_scope("xwait"):
        pltpu.make_async_copy(x_others, x_others, x_recv).wait()
    with jax.named_scope("agsend"):
        total = shares[0:16, :]
        for s in range(1, OWNERS):
            total += shares[s * 16:(s + 1) * 16, :]
        full[pl.ds(slot, 16), :] = total
        zs = [lax.rem(z_at + d, 4) * 16 for d in range(4)]
        ys = [lax.rem(y_at + d, 4) * 4 for d in range(4)]
        xs_ = [lax.rem(x_at + d, 4) for d in range(4)]
        for dz, dy, dx in CUBE_ORDER:
            pltpu.make_async_remote_copy(
                src_ref=mine_rows, dst_ref=mine_rows, send_sem=ag_send, recv_sem=ag_recv.at[group],
                device_id={"sp": zs[dz] + ys[dy] + xs_[dx]}, device_id_type=MESH).start()

    with jax.named_scope("latewait"):
        @pl.when(jnp.logical_and(is_kv, jnp.logical_not(is_last)))
        def _():
            wait_for(2, late_recv)

        @pl.when(jnp.logical_or(jnp.logical_not(is_kv), is_last))
        def _():
            wait_for(3, late_recv)
    with jax.named_scope("update"):
        sub = lax.broadcasted_iota(jnp.int32, (8, 128), 0)

        def update(turn, carry):
            dz = jnp.where(turn == 0, 2, jnp.where(turn == 1, 1, jnp.where(turn == 2, 3, 0)))
            for t in range(2):
                for y in range(4):
                    b = t * 16 + lax.rem(z_at + dz, 4) * 4 + y
                    at = pos_ref[b] - sp * seq_local
                    for i, buf in enumerate((k_buf, v_buf)):
                        new = jnp.zeros((8, 128), F32)
                        for g in range(KV):
                            source = kvs[g, turn, t * 4 + y:t * 4 + y + 1, i * 128:(i + 1) * 128]
                            new = jnp.where(sub % KV == g, source, new)
                        old = buf[b].astype(F32)
                        buf[b] = jnp.concatenate(
                            [jnp.where(sub // KV == at - 2 * v, new, old[v * 8:(v + 1) * 8])
                             for v in range(n_rows // 8)], axis=0).astype(BF16)
            return carry

        lax.fori_loop(0, 4, update, 0)

    def quarter(dx):
        g = lax.rem(group + 4 - dx, KV)
        at = pl.ds(pl.multiple_of(g * quarter_rows, quarter_rows), quarter_rows)
        return g, pltpu.make_async_remote_copy(
            src_ref=full.at[at], dst_ref=other.at[at], send_sem=tp_send.at[g], recv_sem=tp_recv.at[g],
            device_id={"tp": 1 - tp}, device_id_type=MESH)

    def finish(buf, g, core):
        for cb in range(n_cb):
            at = pl.ds(pl.multiple_of((g * 2 + core) * own + cb * 128, 128), 128)
            for t in range(2):
                slab = buf[pl.ds(g * quarter_rows + t * n_cb + cb, n_lines, stride=16), :]
                out_ref[t * 16:(t + 1) * 16, at] = (h_ref[t * 16:(t + 1) * 16, at].astype(F32) + slab).astype(BF16)

    with jax.named_scope("agwait"):
        for dx in QUARTERS:
            g, swap = quarter(dx)
            n = (n_lines if dx else n_lines - 1) * AG_ROWS
            pltpu.make_async_copy(full.at[pl.ds(0, n)], full.at[pl.ds(0, n)], ag_recv.at[g]).wait()
            swap.start()
            finish(full, g, tp)
    with jax.named_scope("swapwait"):
        for dx in QUARTERS:
            g, swap = quarter(dx)
            swap.wait()
            finish(other, g, 1 - tp)

    with jax.named_scope("drain"):
        @pl.when(jnp.logical_and(is_kv, jnp.logical_not(is_last)))
        def _():
            wait_for(4, early_send)

        @pl.when(is_last)
        def _():
            wait_for(3, early_send)

        wait_for_halves(2 * (PLANE - 1), q_send)
        returns = jnp.logical_and(y_at == x_at, jnp.logical_not(is_kv))

        @pl.when(returns)
        def _():
            wait_for(2, late_send)

        @pl.when(jnp.logical_not(returns))
        def _():
            wait_for(3, late_send)

        pltpu.make_async_copy(rs_others, rs_others, rs_send).wait()

        pltpu.make_async_copy(x_others, x_others, x_send).wait()
        f_others = full.at[pl.ds(0, (n_sp - 1) * AG_ROWS)]
        pltpu.make_async_copy(f_others, f_others, ag_send).wait()


def store_kernel(*refs):
    n = len(refs) // 2
    sem = refs[-1]
    copies = [pltpu.make_async_copy(refs[i], refs[n + i], sem.at[i]) for i in range(n)]
    for c in copies:
        c.start()
    for c in copies:
        c.wait()


def solution(mesh):
    cache_spec = P('dp', 'sp', 'tp', None)
    n_sp = mesh.shape["sp"]

    def local_step(hidden, norm_scale, w_qkv, w_out, k_cache, v_cache, positions):
        n_seq, seq_local, kv, head_dim = k_cache.shape
        d_model = hidden.shape[1]
        depth = w_out.shape[0] // kv
        vmem = pl.BlockSpec(memory_space=VMEM)
        hbm = pl.BlockSpec(memory_space=pltpu.HBM)
        half = head_dim // 2
        freq = np.exp(np.arange(half, dtype=np.float32) * np.float32(-2.0 * math.log(500000.0) / head_dim))
        freq = jnp.asarray(np.concatenate([freq, freq])[None].astype(np.float32))
        flat = (n_seq, seq_local * kv, head_dim)
        dma = pltpu.SemaphoreType.DMA

        hidden_type = jax.ShapeDtypeStruct((n_seq, d_model), BF16)
        results = pl.pallas_call(
            step_kernel,
            out_shape=[hidden_type, jax.ShapeDtypeStruct(flat, BF16), jax.ShapeDtypeStruct(flat, BF16)],
            in_specs=[hbm] * 8,
            out_specs=[vmem, vmem, vmem],
            scratch_shapes=[
                pltpu.SMEM((n_seq,), jnp.int32),
                VMEM((n_seq, d_model), BF16),
                VMEM((d_model,), BF16),
                VMEM((1, head_dim), F32),
                dma((4,)),
                VMEM((d_model, head_dim), BF16),
                VMEM((d_model, 2 * head_dim), BF16),
                VMEM((kv // 2, d_model, 4 * head_dim), BF16),
                VMEM((depth, d_model), BF16),
                VMEM((PLANE, 4, 8, head_dim), F32),
                VMEM((kv, 4, 8, 2 * head_dim), F32),
                VMEM((n_seq * 32, head_dim), F32),
                VMEM((n_seq * 32, head_dim), BF16),
                VMEM((n_sp * 16, head_dim), F32),
                VMEM((n_sp * 16, head_dim), F32),
                VMEM((8, depth), F32),
                VMEM((OWNERS * 16, head_dim), F32),
                VMEM((OWNERS * 16, head_dim), F32),
                VMEM((n_sp * 16, head_dim), F32),
                VMEM((n_sp * 16, head_dim), F32),
                dma((K_CHUNKS,)), dma, dma((kv,)), dma((kv,)), dma((2,)), dma, dma((2,)),
            ] + [dma] * 9 + [dma((kv,))] * 3 + [pltpu.SemaphoreType.REGULAR],
            compiler_params=pltpu.CompilerParams(
                collective_id=0, has_side_effects=True, vmem_limit_bytes=48 * 1024 * 1024),
            cost_estimate=pl.CostEstimate(flops=60_000_000_000, bytes_accessed=20_000_000, transcendentals=0),
            name="step",
        )(*[pltpu.with_memory_space_constraint(a, pltpu.HBM) for a in (
            positions, hidden, norm_scale, freq, w_qkv, w_out, k_cache.reshape(flat), v_cache.reshape(flat))])

        h_out, k_new, v_new = pl.pallas_call(
            store_kernel,
            out_shape=[hidden_type, jax.ShapeDtypeStruct(flat, BF16), jax.ShapeDtypeStruct(flat, BF16)],
            in_specs=[vmem] * 3,
            out_specs=[hbm] * 3,
            scratch_shapes=[dma((3,))],
            compiler_params=pltpu.CompilerParams(vmem_limit_bytes=8 * 1024 * 1024),
            name="store",
        )(*[pltpu.with_memory_space_constraint(a, VMEM) for a in results])
        k_new, v_new = k_new.reshape(k_cache.shape), v_new.reshape(v_cache.shape)
        return h_out, k_new, v_new

    return jax.shard_map(
        local_step,
        mesh=mesh,
        in_specs=(P('dp', None), P(None), P(None, 'tp'), P('tp', None), cache_spec, cache_spec, P('dp')),
        out_specs=(P('dp', None), cache_spec, cache_spec),
        check_vma=False,
    )
```

```python
import itertools
import math

import jax
import jax.numpy as jnp
import numpy as np
from jax import lax
from jax.experimental import pallas as pl
from jax.experimental.pallas import tpu as pltpu
from jax.sharding import PartitionSpec as P

MESH = pl.DeviceIdType.MESH
VMEM = pltpu.VMEM
F32 = jnp.float32
BF16 = jnp.bfloat16
NEG = -3.0e38
LEAST = -1.0e38
PLANE = 16
K_CHUNKS = 6
KV = 4
OWNERS = 8
TURNS = (2, 1, 3, 0)
QUARTERS = (0, 1, 3, 2)
RS_ROWS = 13
AG_ROWS = 12


def farthest_first(dims):
    near = lambda o: sum(min(v, 4 - v) for v in o)
    return sorted((o for o in itertools.product(range(4), repeat=dims) if any(o)), key=lambda o: -near(o))


PLANE_ORDER = farthest_first(2)
CUBE_ORDER = farthest_first(3)


def step_kernel(pos_hbm, h_hbm, scale_hbm, freq_hbm, wq_ref, wo_ref, k_ref, v_ref, out_ref, k_buf, v_buf,
                pos_ref, h_ref, scale_ref, freq_ref, in_sem,
                wq_buf, wk_buf, wl_buf, wo_buf, recv, kvs, xs, xb, part, parts, lhs, mine, shares, full, other,
                wq_sem, wk_sem, wl_sem, wo_sem, kv_sem, q_send, q_recv, early_send, early_recv, late_send, late_recv,
                rs_send, rs_recv, x_send, x_recv, ag_send, ag_recv, tp_send, tp_recv, ready):
    sp = lax.axis_index("sp")
    tp = lax.axis_index("tp")
    n_sp = 64
    line, group = lax.div(sp, KV), lax.rem(sp, KV)
    n_lines = n_sp // KV
    j = lax.rem(sp, PLANE)
    base = sp - j
    y_at, x_at = lax.div(j, 4), lax.rem(j, 4)
    z_at = lax.div(sp, PLANE)
    is_kv = x_at == 3
    n_seq, d_model = h_ref.shape
    width = wk_buf.shape[1]
    rows = d_model // K_CHUNKS
    n_rows = k_ref.shape[1]
    seq_local = n_rows // KV
    depth = wo_buf.shape[0]
    own = d_model // OWNERS
    n_cb = own // 128

    def turn_of(dz):
        return jnp.where(dz == 2, 0, jnp.where(dz == 1, 1, jnp.where(dz == 3, 2, 3)))

    wq_at = pl.multiple_of(y_at * 1024 + 256 + x_at * 128, 128)

    def wq_copy(c):
        return pltpu.make_async_copy(
            wq_ref.at[pl.ds(c * rows, rows), pl.ds(wq_at, 128)], wq_buf.at[pl.ds(c * rows, rows)], wq_sem.at[c])

    wk_copy = pltpu.make_async_copy(
        wq_ref.at[:, pl.ds(pl.multiple_of(y_at * 1024 + 768, 256), width)], wk_buf, wk_sem)

    def wl_copy(g):
        return pltpu.make_async_copy(
            wq_ref.at[:, pl.ds(g * 1024, 256)], wl_buf.at[g // 2, :, pl.ds(g % 2 * 256, 256)], wl_sem.at[g])

    def wo_copy(k):
        return pltpu.make_async_copy(
            wo_ref.at[pl.ds(pl.multiple_of(group * depth, depth) + k * (depth // KV), depth // KV)],
            wo_buf.at[pl.ds(k * (depth // KV), depth // KV)], wo_sem.at[k])

    k_copy = pltpu.make_async_copy(k_ref, k_buf, kv_sem.at[0])
    v_copy = pltpu.make_async_copy(v_ref, v_buf, kv_sem.at[1])
    small = [pltpu.make_async_copy(src, dst, in_sem.at[i]) for i, (src, dst) in enumerate(
        [(h_hbm, h_ref), (pos_hbm, pos_ref), (freq_hbm, freq_ref), (scale_hbm, scale_ref)])]
    for c in small:
        c.start()
    barrier = pltpu.get_barrier_semaphore()

    with jax.named_scope("greet"):
        for dy, dx in PLANE_ORDER:
            peer = base + lax.rem(y_at + dy, 4) * 4 + lax.rem(x_at + dx, 4)
            pl.semaphore_signal(barrier, inc=1, device_id={"sp": peer}, device_id_type=MESH)
        for dz in range(1, 4):
            pl.semaphore_signal(barrier, inc=1, device_id={"sp": lax.rem(sp + dz * PLANE, n_sp)}, device_id_type=MESH)
        pl.semaphore_signal(barrier, inc=1, device_id={"tp": 1 - tp}, device_id_type=MESH)
        for c in range(K_CHUNKS):
            wq_copy(c).start()
        pl.when(is_kv)(wk_copy.start)

    with jax.named_scope("hwait"):
        small[0].wait()
        for g in range(KV):
            wl_copy(g).start()
    with jax.named_scope("norm"):
        hidden = h_ref[...].astype(F32)
        centered = hidden - jnp.mean(hidden, axis=-1, keepdims=True)
        var = jnp.mean(centered * centered, axis=-1, keepdims=True)
    with jax.named_scope("inwait"):
        for c in small[1:]:
            c.wait()
    with jax.named_scope("norm2"):
        u = (centered * lax.rsqrt(var + 1e-5) * scale_ref[...].astype(F32)[None, :]).astype(BF16)
        seq_row = lax.broadcasted_iota(jnp.int32, (n_seq, 128), 0)
        pos = jnp.zeros((n_seq, 128), jnp.int32)
        for b in range(n_seq):
            pos = jnp.where(seq_row == b, pos_ref[b], pos)
        angles = pos.astype(F32) * freq_ref[...]
        cos = jnp.cos(angles)
        sin = jnp.sin(angles)
        sin = jnp.where(lax.broadcasted_iota(jnp.int32, (n_seq, 128), 1) < 64, -sin, sin)

    def clipped(product):
        return jnp.clip(product.astype(BF16), -8.0, 8.0).astype(F32)

    def rotate(piece):
        return (piece * cos + pltpu.roll(piece, 64, 1) * sin).astype(BF16).astype(F32)

    def tile_of(y, z):
        return jnp.concatenate([y[z * 4:z * 4 + 4], y[16 + z * 4:16 + z * 4 + 4]], axis=0)

    with jax.named_scope("qkv"):
        accs = [jnp.zeros((n_seq, 128), F32)] * 2
        for c in range(K_CHUNKS):
            wq_copy(c).wait()
            accs[c % 2] += jnp.dot(u[:, c * rows:(c + 1) * rows], wq_buf[c * rows:(c + 1) * rows, :],
                                   preferred_element_type=F32)
        y = rotate(clipped(accs[0] + accs[1]))
        for z in range(4):
            recv[j, turn_of(lax.rem(z + 4 - z_at, 4))] = tile_of(y, z)
    with jax.named_scope("barrier"):
        pl.semaphore_wait(barrier, PLANE - 1 + 3 + 1)

    def to_plane(dy, dx, block, send_sem, recv_sem):
        peer = base + lax.rem(y_at + dy, 4) * 4 + lax.rem(x_at + dx, 4)
        return pltpu.make_async_remote_copy(
            src_ref=block, dst_ref=block, send_sem=send_sem, recv_sem=recv_sem,
            device_id={"sp": peer}, device_id_type=MESH)

    def wait_for(n, sem):
        pltpu.make_async_copy(kvs.at[pl.ds(0, n)], kvs.at[pl.ds(0, n)], sem).wait()

    def wait_for_halves(n, sem):
        flat_half = xs.at[pl.ds(0, n * n_seq // 2)]
        pltpu.make_async_copy(flat_half, flat_half, sem).wait()

    is_last = jnp.logical_and(is_kv, y_at == 3)
    with jax.named_scope("qsend"):
        for dy, dx in PLANE_ORDER:
            to_plane(dy, dx, recv.at[j], q_send, q_recv.at[0]).start()
        for dz in range(1, 4):
            pl.semaphore_signal(ready, inc=1, device_id={"sp": lax.rem(sp + dz * PLANE, n_sp)}, device_id_type=MESH)
        for g in range(KV):
            for r in (6, 7):
                xs[pl.ds(g * 8 + r, n_seq, stride=32), :] = jnp.zeros((n_seq, 128), F32)

    with jax.named_scope("newkv"):
        @pl.when(is_kv)
        def _():
            wk_copy.wait()
            y = clipped(jnp.dot(u, wk_buf[...], preferred_element_type=F32))
            y = jnp.concatenate([rotate(y[:, :128]), y[:, 128:]], axis=1)
            for z in range(4):
                kvs[y_at, turn_of(lax.rem(z + 4 - z_at, 4))] = tile_of(y, z)
            for dy in (2, 1, 3, 0):
                @pl.when(jnp.logical_or(dy != 0, y_at != 3))
                def _():
                    to_plane(dy, lax.rem(y_at + 1, 4), kvs.at[y_at], early_send, early_recv).start()

    with jax.named_scope("local"):
        for pair in range(2):
            wl_copy(pair * 2).wait()
            wl_copy(pair * 2 + 1).wait()
            if pair == 0:
                k_copy.start()
                v_copy.start()
            y = clipped(jnp.dot(u, wl_buf[pair], preferred_element_type=F32))
            for i in range(4):
                piece = rotate(y[:, i * 128:(i + 1) * 128])
                for z in range(4):
                    at = turn_of(lax.rem(z + 4 - z_at, 4)) * 256 + (pair * 2 + i // 2) * 8 + i % 2
                    xs[pl.ds(at, 8, stride=32), :] = tile_of(piece, z)
        for k in range(KV):
            wo_copy(k).start()

    def half_queries(half):
        with jax.named_scope(f"qwait{half}"):
            if half == 0:
                wait_for_halves(2 * (PLANE - 1), q_recv.at[0])
        with jax.named_scope("spread"):
            for turn in (half * 2, half * 2 + 1):
                for blk in range(PLANE):
                    xs[pl.ds(turn * 256 + blk // 4 * 8 + 2 + blk % 4, 8, stride=32), :] = recv[blk, turn]
                xb[turn * 256:(turn + 1) * 256, :] = xs[turn * 256:(turn + 1) * 256, :].astype(BF16)

    row8 = lax.broadcasted_iota(jnp.int32, (32, 128), 0) % 8
    lane32 = lax.broadcasted_iota(jnp.int32, (32, 128), 1)

    def as_rows(cols, n):
        tiles = sum(jnp.where((lane32 == row8 + 8 * t)[:8 * n], c, 0.0) for t, c in enumerate(cols)).reshape(n, 8, 128)
        return jnp.broadcast_to(jnp.sum(tiles, axis=1, keepdims=True), (n, 8, 128)).reshape(8 * n, 128)

    with jax.named_scope("kvwait"):
        k_copy.wait()
        v_copy.wait()
    row = lax.broadcasted_iota(jnp.int32, (32, n_rows), 0)
    col = lax.broadcasted_iota(jnp.int32, (32, n_rows), 1)
    seq_of = jnp.where(col % KV == row // 8, col // KV + sp * seq_local, 1 << 30)
    scale = 128 ** -0.5

    def line_at(turn, i):
        return lax.rem(z_at + TURNS[turn], 4) * 4 + lax.rem(y_at + TURNS[i], 4)

    def scores(turn):
        out = []
        for i in range(4):
            for t in range(2):
                at = (turn * 8 + t * 4 + lax.rem(y_at + TURNS[i], 4)) * 32
                b = line_at(turn, i) + 16 * t
                q = xb[pl.ds(pl.multiple_of(at, 32), 32), :]
                s = lax.dot_general(q, k_buf[b], (((1,), (1,)), ((), ())), preferred_element_type=F32) * scale
                out.append(jnp.where(seq_of < pos_ref[b], s, NEG))
        return out

    def values(turn, held):
        for i in range(4):
            ln = line_at(turn, i)
            stats, outs = [], []
            for t in range(2):
                s = held[i * 2 + t]
                m = jnp.maximum(jnp.max(s, axis=1, keepdims=True), LEAST)
                e = jnp.exp(s - m)
                stats.append((m, jnp.sum(e, axis=1, keepdims=True)))
                outs.append(jnp.dot(e.astype(BF16), v_buf[ln + 16 * t], preferred_element_type=F32))
            (m0, l0), (m1, l1) = stats
            first = jnp.where(row8 == 6, as_rows((m0, m1, l0, l1), KV), outs[0])
            for g in range(KV):
                at = pl.multiple_of((ln * KV + g) * 16, 16)
                part[pl.ds(at, 8), :] = first[g * 8:(g + 1) * 8]
                part[pl.ds(at + 7, 6), :] = outs[1][g * 8:g * 8 + 6]

    def send_partials(turn):
        for i in range(4):
            ln = line_at(turn, i)
            for d in TURNS:
                if turn == 3 and i == 3 and d == 0:
                    continue
                to = lax.rem(group + d, KV)
                pltpu.make_async_remote_copy(
                    src_ref=part.at[pl.ds(pl.multiple_of((ln * KV + to) * 16, 16), RS_ROWS)],
                    dst_ref=parts.at[pl.ds(pl.multiple_of(sp * 16, 16), RS_ROWS)], send_sem=rs_send,
                    recv_sem=rs_recv, device_id={"sp": ln * KV + to}, device_id_type=MESH).start()

    half_queries(0)
    with jax.named_scope("ready"):
        pl.semaphore_wait(ready, 3)
    with jax.named_scope("attn0"):
        held = scores(0)
        ahead = scores(1)
        values(0, held)
        send_partials(0)
        values(1, ahead)
        send_partials(1)
    half_queries(1)
    with jax.named_scope("attn1"):
        held = scores(2)
        ahead = scores(3)
        values(2, held)
        send_partials(2)
        values(3, ahead)
        send_partials(3)
        parts[pl.ds(pl.multiple_of(sp * 16, 16), 16), :] = part[pl.ds(pl.multiple_of(sp * 16, 16), 16), :]

    with jax.named_scope("newrow"):
        @pl.when(jnp.logical_not(is_last))
        def _():
            wait_for(1, early_recv)

        for i in range(2):
            xs[pl.ds(3 * 256 + group * 8 + 6 + i, 8, stride=32), :] = kvs[group, 3, :, i * 128:(i + 1) * 128]
        cols, v_new = [], []
        for t in range(2):
            tile = xs[pl.ds(pl.multiple_of((24 + t * 4 + y_at) * 32 + group * 8, 8), 8), :]
            cols.append(jnp.sum(tile * tile[6:7, :], axis=1, keepdims=True) * scale)
            v_new.append(tile[7:8, :])
        m_new = as_rows(cols, 1)[:1]

    rs_others = parts.at[pl.ds(0, (n_sp - 1) * RS_ROWS)]
    with jax.named_scope("rswait"):
        pltpu.make_async_copy(rs_others, rs_others, rs_recv).wait()

    with jax.named_scope("merge"):
        lane = lax.broadcasted_iota(jnp.int32, (1, 128), 1)
        m = parts[pl.ds(6, n_sp, stride=16), :]
        l = pltpu.roll(m, 112, 1)
        top = jnp.maximum(jnp.max(m, axis=0, keepdims=True), m_new)
        f = jnp.exp(m - top)
        f_new = jnp.exp(m_new - top)
        real = jnp.logical_and(lane < 16, lane % 8 < 6)
        den = jnp.where(real, jnp.sum(f * l, axis=0, keepdims=True) + f_new, 1.0)
        wt = (jnp.concatenate([f, jnp.broadcast_to(f_new, (8, 128))], axis=0) / den).T
        lhs[...] = jnp.zeros_like(lhs)
        for t in range(2):
            w8 = wt[t * 8:(t + 1) * 8]
            sums = [w8[:, n_sp:n_sp + 1] * v_new[t]] + [jnp.zeros((8, 128), F32)] * 3
            for s in range(n_sp):
                sums[s % 4] += w8[:, s:s + 1] * parts[s * 16 + t * 7:s * 16 + t * 7 + 8, :]
            acc = (sums[0] + sums[1]) + (sums[2] + sums[3])
            for hd in range(6):
                lhs[t:t + 1, hd * 128:(hd + 1) * 128] = acc[hd:hd + 1, :]

    me = group * 2 + tp
    with jax.named_scope("wout"):
        for k in range(KV):
            wo_copy(k).wait()
        left = lhs[...].astype(BF16)

        order = [(dg, dt) for dg in TURNS for dt in (1, 0)]

        def product(k):
            owner = lax.rem(group + order[k][0], KV) * 2 + (1 - tp if order[k][1] else tp)
            at = pl.multiple_of(owner * own, own)
            return owner, jnp.dot(left, wo_buf[:, pl.ds(at, own)], preferred_element_type=F32)

        held = product(0)
        for k in range(OWNERS):
            ahead = product(k + 1) if k + 1 < OWNERS else None
            owner, res = held
            buf = mine if k < OWNERS - 1 else shares
            at = pl.multiple_of(owner * 16, 16)
            for t in range(2):
                for cb in range(n_cb):
                    buf[pl.ds(at + t * n_cb + cb, 1), :] = res[t:t + 1, cb * 128:(cb + 1) * 128]
            if k < OWNERS - 1:
                pltpu.make_async_remote_copy(
                    src_ref=mine.at[pl.ds(at, AG_ROWS)],
                    dst_ref=shares.at[pl.ds(pl.multiple_of(me * 16, 16), AG_ROWS)], send_sem=x_send, recv_sem=x_recv,
                    device_id={"tp": lax.rem(owner, 2), "sp": line * KV + lax.div(owner, 2)},
                    device_id_type=MESH).start()
            held = ahead

    with jax.named_scope("forward"):
        for dx in (2, 1, 3):
            to = lax.rem(x_at + dx, 4)

            @pl.when(jnp.logical_or(to != 3, y_at != x_at))
            def _():
                pltpu.make_async_remote_copy(
                    src_ref=kvs.at[group], dst_ref=kvs.at[group], send_sem=late_send,
                    recv_sem=late_recv, device_id={"sp": line * 4 + to}, device_id_type=MESH).start()

    x_others = shares.at[pl.ds(0, (OWNERS - 1) * AG_ROWS)]
    quarter_rows = n_lines * 16
    slot = pl.multiple_of((group * n_lines + line) * 16, 16)
    mine_rows = full.at[pl.ds(slot, AG_ROWS)]

    with jax.named_scope("xwait"):
        pltpu.make_async_copy(x_others, x_others, x_recv).wait()
    with jax.named_scope("agsend"):
        total = shares[0:16, :]
        for s in range(1, OWNERS):
            total += shares[s * 16:(s + 1) * 16, :]
        full[pl.ds(slot, 16), :] = total
        zs = [lax.rem(z_at + d, 4) * 16 for d in range(4)]
        ys = [lax.rem(y_at + d, 4) * 4 for d in range(4)]
        xs_ = [lax.rem(x_at + d, 4) for d in range(4)]
        for dz, dy, dx in CUBE_ORDER:
            pltpu.make_async_remote_copy(
                src_ref=mine_rows, dst_ref=mine_rows, send_sem=ag_send, recv_sem=ag_recv.at[group],
                device_id={"sp": zs[dz] + ys[dy] + xs_[dx]}, device_id_type=MESH).start()

    with jax.named_scope("latewait"):
        @pl.when(jnp.logical_and(is_kv, jnp.logical_not(is_last)))
        def _():
            wait_for(2, late_recv)

        @pl.when(jnp.logical_or(jnp.logical_not(is_kv), is_last))
        def _():
            wait_for(3, late_recv)
    with jax.named_scope("update"):
        sub = lax.broadcasted_iota(jnp.int32, (8, 128), 0)

        def update(turn, carry):
            dz = jnp.where(turn == 0, 2, jnp.where(turn == 1, 1, jnp.where(turn == 2, 3, 0)))
            for t in range(2):
                for y in range(4):
                    b = t * 16 + lax.rem(z_at + dz, 4) * 4 + y
                    at = pos_ref[b] - sp * seq_local
                    for i, buf in enumerate((k_buf, v_buf)):
                        new = jnp.zeros((8, 128), F32)
                        for g in range(KV):
                            source = kvs[g, turn, t * 4 + y:t * 4 + y + 1, i * 128:(i + 1) * 128]
                            new = jnp.where(sub % KV == g, source, new)
                        old = buf[b].astype(F32)
                        buf[b] = jnp.concatenate(
                            [jnp.where(sub // KV == at - 2 * v, new, old[v * 8:(v + 1) * 8])
                             for v in range(n_rows // 8)], axis=0).astype(BF16)
            return carry

        lax.fori_loop(0, 4, update, 0)

    def quarter(dx):
        g = lax.rem(group + 4 - dx, KV)
        at = pl.ds(pl.multiple_of(g * quarter_rows, quarter_rows), quarter_rows)
        return g, pltpu.make_async_remote_copy(
            src_ref=full.at[at], dst_ref=other.at[at], send_sem=tp_send.at[g], recv_sem=tp_recv.at[g],
            device_id={"tp": 1 - tp}, device_id_type=MESH)

    def finish(buf, g, core):
        for cb in range(n_cb):
            at = pl.ds(pl.multiple_of((g * 2 + core) * own + cb * 128, 128), 128)
            for t in range(2):
                slab = buf[pl.ds(g * quarter_rows + t * n_cb + cb, n_lines, stride=16), :]
                out_ref[t * 16:(t + 1) * 16, at] = (h_ref[t * 16:(t + 1) * 16, at].astype(F32) + slab).astype(BF16)

    with jax.named_scope("agwait"):
        for dx in QUARTERS:
            g, swap = quarter(dx)
            n = (n_lines if dx else n_lines - 1) * AG_ROWS
            pltpu.make_async_copy(full.at[pl.ds(0, n)], full.at[pl.ds(0, n)], ag_recv.at[g]).wait()
            swap.start()
            finish(full, g, tp)
    with jax.named_scope("swapwait"):
        for dx in QUARTERS:
            g, swap = quarter(dx)
            swap.wait()
            finish(other, g, 1 - tp)

    with jax.named_scope("drain"):
        @pl.when(jnp.logical_and(is_kv, jnp.logical_not(is_last)))
        def _():
            wait_for(4, early_send)

        @pl.when(is_last)
        def _():
            wait_for(3, early_send)

        wait_for_halves(2 * (PLANE - 1), q_send)
        returns = jnp.logical_and(y_at == x_at, jnp.logical_not(is_kv))

        @pl.when(returns)
        def _():
            wait_for(2, late_send)

        @pl.when(jnp.logical_not(returns))
        def _():
            wait_for(3, late_send)

        pltpu.make_async_copy(rs_others, rs_others, rs_send).wait()

        pltpu.make_async_copy(x_others, x_others, x_send).wait()
        f_others = full.at[pl.ds(0, (n_sp - 1) * AG_ROWS)]
        pltpu.make_async_copy(f_others, f_others, ag_send).wait()


def store_kernel(*refs):
    n = len(refs) // 2
    sem = refs[-1]
    copies = [pltpu.make_async_copy(refs[i], refs[n + i], sem.at[i]) for i in range(n)]
    for c in copies:
        c.start()
    for c in copies:
        c.wait()


def solution(mesh):
    cache_spec = P('dp', 'sp', 'tp', None)
    n_sp = mesh.shape["sp"]

    def local_step(hidden, norm_scale, w_qkv, w_out, k_cache, v_cache, positions):
        n_seq, seq_local, kv, head_dim = k_cache.shape
        d_model = hidden.shape[1]
        depth = w_out.shape[0] // kv
        vmem = pl.BlockSpec(memory_space=VMEM)
        hbm = pl.BlockSpec(memory_space=pltpu.HBM)
        half = head_dim // 2
        freq = np.exp(np.arange(half, dtype=np.float32) * np.float32(-2.0 * math.log(500000.0) / head_dim))
        freq = jnp.asarray(np.concatenate([freq, freq])[None].astype(np.float32))
        flat = (n_seq, seq_local * kv, head_dim)
        dma = pltpu.SemaphoreType.DMA

        hidden_type = jax.ShapeDtypeStruct((n_seq, d_model), BF16)
        results = pl.pallas_call(
            step_kernel,
            out_shape=[hidden_type, jax.ShapeDtypeStruct(flat, BF16), jax.ShapeDtypeStruct(flat, BF16)],
            in_specs=[hbm] * 8,
            out_specs=[vmem, vmem, vmem],
            scratch_shapes=[
                pltpu.SMEM((n_seq,), jnp.int32),
                VMEM((n_seq, d_model), BF16),
                VMEM((d_model,), BF16),
                VMEM((1, head_dim), F32),
                dma((4,)),
                VMEM((d_model, head_dim), BF16),
                VMEM((d_model, 2 * head_dim), BF16),
                VMEM((kv // 2, d_model, 4 * head_dim), BF16),
                VMEM((depth, d_model), BF16),
                VMEM((PLANE, 4, 8, head_dim), F32),
                VMEM((kv, 4, 8, 2 * head_dim), F32),
                VMEM((n_seq * 32, head_dim), F32),
                VMEM((n_seq * 32, head_dim), BF16),
                VMEM((n_sp * 16, head_dim), F32),
                VMEM((n_sp * 16, head_dim), F32),
                VMEM((8, depth), F32),
                VMEM((OWNERS * 16, head_dim), F32),
                VMEM((OWNERS * 16, head_dim), F32),
                VMEM((n_sp * 16, head_dim), F32),
                VMEM((n_sp * 16, head_dim), F32),
                dma((K_CHUNKS,)), dma, dma((kv,)), dma((kv,)), dma((2,)), dma, dma((2,)),
            ] + [dma] * 9 + [dma((kv,))] * 3 + [pltpu.SemaphoreType.REGULAR],
            compiler_params=pltpu.CompilerParams(
                collective_id=0, has_side_effects=True, vmem_limit_bytes=48 * 1024 * 1024),
            cost_estimate=pl.CostEstimate(flops=60_000_000_000, bytes_accessed=20_000_000, transcendentals=0),
            name="step",
        )(*[pltpu.with_memory_space_constraint(a, pltpu.HBM) for a in (
            positions, hidden, norm_scale, freq, w_qkv, w_out, k_cache.reshape(flat), v_cache.reshape(flat))])

        h_out, k_new, v_new = pl.pallas_call(
            store_kernel,
            out_shape=[hidden_type, jax.ShapeDtypeStruct(flat, BF16), jax.ShapeDtypeStruct(flat, BF16)],
            in_specs=[vmem] * 3,
            out_specs=[hbm] * 3,
            scratch_shapes=[dma((3,))],
            compiler_params=pltpu.CompilerParams(vmem_limit_bytes=8 * 1024 * 1024),
            name="store",
        )(*[pltpu.with_memory_space_constraint(a, VMEM) for a in results])
        k_new, v_new = k_new.reshape(k_cache.shape), v_new.reshape(v_cache.shape)
        return h_out, k_new, v_new

    return jax.shard_map(
        local_step,
        mesh=mesh,
        in_specs=(P('dp', None), P(None), P(None, 'tp'), P('tp', None), cache_spec, cache_spec, P('dp')),
        out_specs=(P('dp', None), cache_spec, cache_spec),
        check_vma=False,
    )
```
